128 devices in a mesh: gx: 4 (over x_hi, core), gy: 4 (over y), gz: 8 (over z, x_lo).
Axes of the slice: x: 4 (x_hi: 2, x_lo: 2; x = x_hi * 2 + x_lo), y: 4, z: 4, core: 2. Of those that a mesh axis runs over, the one named last changes fastest.
Arguments:
- field: float32 [64, 1024, 1024], P('gx', 'gy', 'gz'), may hold values from -6 to 6
- source: float32 [64, 1024, 1024], P('gx', 'gy', 'gz'), may hold values from -6 to 6
Outputs:
- smoothed: float32 [64, 1024, 1024], P('gx', 'gy', 'gz')
The draws below stay inside these ranges and needn't reach their ends.
All inputs are finite; a program needn't handle non-finite values.
Results may differ from the reference program's by a relative error of at most 0.00002.
Values sent between devices are 32-bit elements; how exact they have to be, the bound alone decides.
A program may use at most 64 MiB of HBM per device.

```python
import jax
import jax.numpy as jnp

SWEEPS = 3
NX = 64
NY = 1024
NZ = 1024


def block_levels(key, shape, split, least, top_value):
    def one(position, parts):
        draws = jax.random.uniform(jax.random.fold_in(jax.random.fold_in(key, 6), position), (parts,), jnp.float32, least / len(split), top_value / len(split))
        return jnp.repeat(jnp.exp(draws), shape[position] // parts).reshape((-1,) + (1,) * (len(shape) - position - 1))

    loudness = one(*split[0])
    for cut in split[1:]:
        loudness = loudness * one(*cut)
    return loudness


def bell_draw(own_key, shape, spread, most, shards=(), held_as=jnp.bfloat16):
    entries = jax.random.normal(own_key, shape, jnp.float32) * spread
    if len(shards) > 0:
        entries = block_levels(own_key, shape, shards, -0.22, 0.18) * entries
    return jnp.clip(entries, min=-most, max=most).astype(held_as)


def setup_inputs(seed: int = 0) -> dict:
    key_of = jax.random.split(jax.random.key(seed), 3)
    field = bell_draw(key_of[0], (NX, NY, NZ), 1.0, 6.0, ((0, 4), (1, 4), (2, 8)), jnp.float32)
    source = bell_draw(key_of[1], (NX, NY, NZ), 1.0, 6.0, ((0, 4), (1, 4), (2, 8)), jnp.float32)
    return dict(field=field, source=source)


def relax(values, source, parity, colour):
    padded = jnp.pad(values, ((1, 1), (0, 0), (0, 0)))
    beside = padded[2:] + padded[:-2]
    beside = beside + jnp.roll(values, -1, 1) + jnp.roll(values, 1, 1)
    beside = beside + jnp.roll(values, -1, 2) + jnp.roll(values, 1, 2)
    return jnp.where(parity == colour, (source + beside) / 6.0, values)


def reference(field, source):
    nx, ny, nz = field.shape
    parity = (jnp.arange(nx, dtype=jnp.int32)[:, None, None] + jnp.arange(ny, dtype=jnp.int32)[None, :, None] + jnp.arange(nz, dtype=jnp.int32)[None, None, :]) % 2
    values = field
    for sweep in range(SWEEPS):
        values = relax(values, source, parity, 0)
        values = relax(values, source, parity, 1)
    return values
```

```python
import functools

import jax
import jax.numpy as jnp
from jax import lax
from jax.experimental import pallas as pl
from jax.experimental.pallas import tpu as pltpu
from jax.sharding import PartitionSpec as P

SWEEPS = 3
HALF = 2 * SWEEPS
PAD = 16
LANES = 128
CHUNK = 8
MESH = pl.DeviceIdType.MESH


def iota(shape, dim):
    return lax.broadcasted_iota(jnp.int32, shape, dim)


def kernel(field, source, out, fbuf, sbuf, obuf, S, X, own, zbuf, isem, osem, ssem, rsem):
    M = X.shape[1] - 2
    N = X.shape[2] - 2 * PAD
    T = N // 8
    gx, gy, gz = (lax.axis_index(a) for a in ("gx", "gy", "gz"))
    nx, ny, nz = (lax.axis_size(a) for a in ("gx", "gy", "gz"))
    up = lambda i, n: lax.rem(i + 1, n)
    down = lambda i, n: lax.rem(i + n - 1, n)
    targets = (
        {"gx": down(gx, nx)}, {"gx": up(gx, nx)},
        {"gy": down(gy, ny)}, {"gy": up(gy, ny)},
        {"gz": down(gz, nz)}, {"gz": up(gz, nz)},
    )
    has_low, has_high = gx > 0, gx < nx - 1
    sends = (has_low, has_high, None, None, None, None)
    gets = (has_high, has_low, None, None, None, None)

    def guarded(condition, action):
        if condition is None:
            action()
        else:
            pl.when(condition)(action)

    planes = 2 * M // 4
    loads = []
    for part, first in enumerate((0, 3, 1, 2) if 2 * M >= 16 else range(4)):
        here = pl.ds(first * planes, planes)
        loads.append(pltpu.make_async_copy(field.at[here], fbuf.at[here], isem.at[0, part]))
    for part in range(4):
        here = pl.ds(part * planes, planes)
        loads.append(pltpu.make_async_copy(source.at[here], sbuf.at[here], isem.at[1, part]))
    for load in loads:
        load.start()

    barrier = pltpu.get_barrier_semaphore()
    for condition, target in zip(sends, targets):
        guarded(condition, functools.partial(
            pl.semaphore_signal, barrier, inc=1, device_id=target, device_id_type=MESH))

    rows = pl.ds(PAD, N)
    inner = pl.ds(1, M)

    def copies(h):
        pairs = (
            (X.at[h, 1, rows], X.at[h, M + 1, rows]),
            (X.at[h, M, rows], X.at[h, 0, rows]),
            (X.at[h, inner, pl.ds(PAD, 8)], X.at[h, inner, pl.ds(PAD + N, 8)]),
            (X.at[h, inner, pl.ds(PAD + N - 8, 8)], X.at[h, inner, pl.ds(PAD - 8, 8)]),
            (own.at[h], zbuf.at[h, 1]),
            (own.at[h], zbuf.at[h, 0]),
        )
        return [
            pltpu.make_async_remote_copy(
                src_ref=src, dst_ref=dst, send_sem=ssem.at[h, d], recv_sem=rsem.at[h, d],
                device_id=targets[d], device_id_type=MESH)
            for d, (src, dst) in enumerate(pairs)
        ]

    lane = iota((8, LANES), 1)
    group = lane // 4
    place = lane % 4
    odd = (iota((N, LANES), 0) + iota((N, LANES), 1)) % 2 == 1
    odd_chunk = (iota((8 * CHUNK, LANES), 0) + iota((8 * CHUNK, LANES), 1)) % 2 == 1
    lane_chunk = iota((8 * CHUNK, LANES), 1)

    zero = jnp.zeros((N, LANES), jnp.float32)

    @pl.when(gx == 0)
    def _():
        for h in range(HALF):
            X[h, 0, rows] = zero

    @pl.when(gx == nx - 1)
    def _():
        for h in range(HALF):
            X[h, M + 1, rows] = zero

    for load in loads[:4]:
        load.wait()

    def pack(acc, t, value):
        return jnp.where(group == t, pltpu.roll(value, (4 * t + 2) % LANES, 1), acc)

    @pl.loop(0, M)
    def _(m):
        value = jnp.where(odd, fbuf[2 * m], fbuf[2 * m + 1])
        X[0, m + 1, rows] = value
        acc = jnp.zeros((8, LANES), jnp.float32)
        for t in range(T):
            acc = pack(acc, t, value[8 * t:8 * t + 8])
        own[0, m] = acc

    pl.semaphore_wait(barrier, 4 + has_low.astype(jnp.int32) + has_high.astype(jnp.int32))

    def start(h):
        for condition, copy in zip(sends, copies(h)):
            guarded(condition, copy.start)

    def wait(h):
        for condition, copy in zip(gets, copies(h)):
            guarded(condition, copy.wait_recv)

    start(0)
    for load in loads[4:]:
        load.wait()

    @pl.loop(0, M)
    def _(m):
        even_plane, odd_plane = sbuf[2 * m], sbuf[2 * m + 1]
        S[0, m] = jnp.where(odd, odd_plane, even_plane)
        S[1, m] = jnp.where(odd, even_plane, odd_plane)

    for h in range(HALF):
        colour = h % 2
        wait(h)

        @pl.loop(0, M)
        def _(m):
            edge = jnp.where(place == 1, zbuf[h, 0, m], pltpu.roll(zbuf[h, 1, m], LANES - 2, 1))
            acc = jnp.zeros((8, LANES), jnp.float32)
            for first in range(0, T, CHUNK):
                tiles = range(first, min(first + CHUNK, T))
                length = 8 * len(tiles)
                start_row = PAD + 8 * first
                here = pl.ds(start_row, length)
                centre = X[h, m + 1, here]
                before, after = X[h, m, here], X[h, m + 2, here]
                if colour == 0:
                    beside = jnp.where(odd_chunk[:length], after, before)
                else:
                    beside = jnp.where(odd_chunk[:length], before, after)
                wings = jnp.concatenate(
                    [pltpu.roll(edge, (LANES - 1 - 4 * t) % LANES, 1) for t in tiles], 0)
                lanes = lane_chunk[:length]
                left = jnp.where(lanes == 0, wings, pltpu.roll(centre, 1, 1))
                right = jnp.where(lanes == LANES - 1, wings, pltpu.roll(centre, LANES - 1, 1))
                total = (S[colour, m, pl.ds(8 * first, length)] + centre) + (beside + (left + right))
                total = total + (X[h, m + 1, pl.ds(start_row - 1, length)]
                                 + X[h, m + 1, pl.ds(start_row + 1, length)])
                value = total * jnp.float32(1.0 / 6.0)
                if h < HALF - 1:
                    X[h + 1, m + 1, here] = value
                    for t in tiles:
                        acc = pack(acc, t, value[8 * (t - first):8 * (t - first) + 8])
                else:
                    spot = pl.ds(8 * first, length)
                    obuf[2 * m, spot] = jnp.where(odd_chunk[:length], value, centre)
                    obuf[2 * m + 1, spot] = jnp.where(odd_chunk[:length], centre, value)
            if h < HALF - 1:
                own[h + 1, m] = acc

        if h < HALF - 1:
            start(h + 1)

    store = pltpu.make_async_copy(obuf, out, osem)
    store.start()
    for h in range(HALF):
        for condition, copy in zip(sends, copies(h)):
            guarded(condition, copy.wait_send)
    store.wait()


def on_device(field, source):
    L, N, K = field.shape
    M = L // 2
    f32 = jnp.float32
    return pl.pallas_call(
        kernel,
        out_shape=jax.ShapeDtypeStruct(field.shape, f32),
        in_specs=[pl.BlockSpec(memory_space=pl.ANY)] * 2,
        out_specs=pl.BlockSpec(memory_space=pl.ANY),
        scratch_shapes=[
            pltpu.VMEM((L, N, K), f32),
            pltpu.VMEM((L, N, K), f32),
            pltpu.VMEM((L, N, K), f32),
            pltpu.VMEM((2, M, N, K), f32),
            pltpu.VMEM((HALF, M + 2, N + 2 * PAD, K), f32),
            pltpu.VMEM((HALF, M, 8, K), f32),
            pltpu.VMEM((HALF, 2, M, 8, K), f32),
            pltpu.SemaphoreType.DMA((2, 4)),
            pltpu.SemaphoreType.DMA,
            pltpu.SemaphoreType.DMA((HALF, 6)),
            pltpu.SemaphoreType.DMA((HALF, 6)),
        ],
        compiler_params=pltpu.CompilerParams(collective_id=0, has_side_effects=True),
    )(field, source)


def solution(mesh):
    spec = P("gx", "gy", "gz")
    return jax.shard_map(on_device, mesh=mesh, in_specs=(spec, spec), out_specs=spec, check_vma=False)
```

```python
import functools
import itertools

import jax
import jax.numpy as jnp
from jax import lax
from jax.experimental import pallas as pl
from jax.experimental.pallas import tpu as pltpu
from jax.sharding import PartitionSpec as P

SWEEPS = 3
HALF = 2 * SWEEPS
PAD = 16
LANES = 128
CHUNK = 8
SIXTH = 1.0 / 6.0
MESH = pl.DeviceIdType.MESH
AXES = ("gx", "gy", "gz")
ROUTES = [r for r in itertools.product((-1, 0, 1), repeat=3) if 1 <= sum(map(abs, r)) <= 2]
f32 = jnp.float32
bf16 = jnp.bfloat16


def iota(shape, dim):
    return lax.broadcasted_iota(jnp.int32, shape, dim)


def side(step):
    return 0 if step < 0 else 1


def kernel(field, source, out, fbuf, sbuf, obuf, S, X, own, zout, zin, xzin, yzout, yzin,
           sown, szin, SC, C, U, Y, isem, osem, ssem, rsem):
    M = X.shape[1] - 2
    N = X.shape[2] - 2 * PAD
    T = N // 8
    H = M // 2
    at = {a: lax.axis_index(a) for a in AXES}
    size = {a: lax.axis_size(a) for a in AXES}
    has = (at["gx"] > 0, at["gx"] < size["gx"] - 1)

    def target(route):
        return {a: lax.rem(at[a] + step + size[a], size[a]) for a, step in zip(AXES, route) if step}

    def guarded(step, action):
        if step == 0:
            action()
        else:
            pl.when(has[side(step)])(action)

    rows = pl.ds(PAD, N)
    inner = pl.ds(1, M)
    first, last = pl.ds(PAD, 8), pl.ds(PAD + N - 8, 8)
    before, after = pl.ds(PAD - 8, 8), pl.ds(PAD + N, 8)
    edge_rows = ((first, after), (last, before))

    def refs(r, route):
        x, y, z = route
        h = 2 * r
        if x:
            src_plane, dst_plane = ((1, M + 1), (M, 0))[side(x)]
        if y:
            src_rows, dst_rows = edge_rows[side(y)]
        if x and y:
            return X.at[h, src_plane, src_rows], X.at[h, dst_plane, dst_rows]
        if x and z:
            return own.at[r, src_plane - 1], xzin.at[r, side(-x), side(-z)]
        if y and z:
            return yzout.at[r, side(y)], yzin.at[r, side(-y), side(-z)]
        if x:
            return X.at[h, src_plane, rows], X.at[h, dst_plane, rows]
        if y:
            return X.at[h, inner, src_rows], X.at[h, inner, dst_rows]
        return zout.at[r, side(z)], zin.at[r, side(-z)]

    def source_refs(route):
        x, y, z = route
        if x:
            src_plane, dst_plane = ((1, M + 1), (M, 0))[side(x)]
            return S.at[0, src_plane, rows], S.at[0, dst_plane, rows]
        if y:
            src_rows, dst_rows = edge_rows[side(y)]
            return S.at[0, inner, src_rows], S.at[0, inner, dst_rows]
        return sown, szin.at[side(-z)]

    def remote(r, route):
        pair = refs(r, route) if r < SWEEPS else source_refs(route)
        number = ROUTES.index(route)
        return pltpu.make_async_remote_copy(
            src_ref=pair[0], dst_ref=pair[1], send_sem=ssem.at[r, number], recv_sem=rsem.at[r, number],
            device_id=target(route), device_id_type=MESH)

    faces = [r for r in ROUTES if sum(map(abs, r)) == 1]

    def start(r, routes):
        for route in routes:
            guarded(route[0], lambda route=route: remote(r, route).start())

    def wait(r, routes):
        for route in routes:
            guarded(-route[0], lambda route=route: remote(r, route).wait_recv())

    planes = 2 * M // 4
    loads = []
    for slot, (big, small) in enumerate(((field, fbuf), (source, sbuf))):
        for part in (0, 3, 1, 2):
            here = pl.ds(part * planes, planes)
            loads.append(pltpu.make_async_copy(big.at[here], small.at[here], isem.at[slot, part]))
    for load in loads:
        load.start()
    barrier = pltpu.get_barrier_semaphore()
    count = jnp.int32(0)
    for route in ROUTES:
        guarded(route[0], lambda route=route: pl.semaphore_signal(
            barrier, inc=1, device_id=target(route), device_id_type=MESH))
        count = count + (1 if route[0] == 0 else has[side(route[0])].astype(jnp.int32))

    lane = iota((8, LANES), 1)
    sub = iota((8, LANES), 0)
    group = lane // 4
    place = lane % 4
    odd8 = (sub + lane) % 2 == 1
    outer = (lane == 0) | (lane == LANES - 1)
    odd_rows = (iota((8 * CHUNK, LANES), 0) + iota((8 * CHUNK, LANES), 1)) % 2 == 1
    outer_rows = (iota((8 * CHUNK, LANES), 1) == 0) | (iota((8 * CHUNK, LANES), 1) == LANES - 1)
    gap = jnp.abs(iota((LANES, LANES), 0) - iota((LANES, LANES), 1))
    beside_lanes = jnp.where(gap == 1, 1.0, 0.0).astype(bf16)
    beside_lanes = jnp.concatenate([beside_lanes, beside_lanes], 0)

    def turn(value, shift, axis=1):
        return pltpu.roll(value, shift % value.shape[axis], axis)

    def lane_sum(value):
        high = value.astype(bf16)
        rest = (value - high.astype(f32)).astype(bf16)
        return jnp.dot(jnp.concatenate([high, rest], 1), beside_lanes, preferred_element_type=f32)

    def swapped(value):
        where = iota(value.shape, 1) % 4
        return jnp.where(where == 1, turn(value, -1), turn(value, 1))

    def pack(acc, t, tile):
        return jnp.where(group == t, turn(tile, 4 * t + 2), acc)

    @pl.when(at["gx"] == 0)
    def _():
        for h in range(HALF):
            X[h, 0] = jnp.zeros(X.shape[2:], f32)
        for r in range(SWEEPS):
            xzin[r, 0] = jnp.zeros(xzin.shape[2:], f32)

    @pl.when(at["gx"] == size["gx"] - 1)
    def _():
        for h in range(HALF):
            X[h, M + 1] = jnp.zeros(X.shape[2:], f32)
        for r in range(SWEEPS):
            xzin[r, 1] = jnp.zeros(xzin.shape[2:], f32)

    def finish_pack(r):
        for m in range(H):
            one, two = own[r, m], own[r, m + H]
            zout[r, 0, m] = jnp.where(place >= 2, one, turn(two, -2))
            zout[r, 1, m] = jnp.where(place < 2, one, turn(two, 2))
        for m in range(M):
            yzout[r, 0, m:m + 1] = own[r, m, 0:1]
            yzout[r, 1, m:m + 1] = own[r, m, 7:8]

    order = [0, M - 1] + list(range(1, M - 1))
    x_routes = [r for r in ROUTES if r[0]]
    other_routes = [r for r in ROUTES if not r[0]]
    whole_odd = (iota((N, LANES), 0) + iota((N, LANES), 1)) % 2 == 1

    for load in loads[:4]:
        load.wait()
    for m in order:
        value = jnp.where(whole_odd, fbuf[2 * m], fbuf[2 * m + 1])
        X[0, m + 1, rows] = value
        acc = jnp.zeros((8, LANES), f32)
        for t in range(T):
            acc = pack(acc, t, value[8 * t:8 * t + 8])
        own[0, m] = acc
    finish_pack(0)
    pl.semaphore_wait(barrier, count)
    start(0, ROUTES)

    for load in loads[4:]:
        load.wait()
    for m in order:
        even_plane, odd_plane = sbuf[2 * m], sbuf[2 * m + 1]
        value = jnp.where(whole_odd, odd_plane, even_plane)
        S[0, m + 1, rows] = value
        S[1, m + 1, rows] = jnp.where(whole_odd, even_plane, odd_plane)
        acc = jnp.zeros((8, LANES), f32)
        for t in (range(T)):
            acc = pack(acc, t, value[8 * t:8 * t + 8])
        sown[m] = acc
    start(SWEEPS, faces)

    def update(h, m, start_row, length, wings, near=None):
        here = pl.ds(start_row, length)
        centre = X[h, m + 1, here]
        if near is None:
            low, high = X[h, m, here], X[h, m + 2, here]
            if h % 2:
                low, high = high, low
            near = jnp.where(odd_rows[:length], high, low)
        else:
            near = X[h, near + 1, here]
        total = (S[h % 2, m + 1, here] + centre) + (near + lane_sum(centre))
        total = total + (X[h, m + 1, pl.ds(start_row - 1, length)] + X[h, m + 1, pl.ds(start_row + 1, length)])
        return (total + jnp.where(outer_rows[:length], wings, 0.0)) * f32(SIXTH)

    def wings_of(edge, tiles):
        return jnp.concatenate([turn(edge, LANES - 2 - 4 * t) for t in tiles], 0)

    chunks = [range(c, min(c + CHUNK, T)) for c in range(0, T, CHUNK)]

    for r in range(SWEEPS):
        h = 2 * r
        wait(r, ROUTES)
        if r == 0:
            wait(SWEEPS, faces)
            for m in range(M):
                SC[m] = jnp.where(place == 1, szin[0, m], szin[1, m])
        for m in range(M):
            a, b = zin[r, 0, m % H], zin[r, 1, m % H]
            if m >= H:
                a, b = turn(a, -2), turn(b, 2)
            C[m + 1] = jnp.where(place == 1, a, b)
        C[0] = jnp.where(place == 1, xzin[r, 0, 0], xzin[r, 0, 1])
        C[M + 1] = jnp.where(place == 1, xzin[r, 1, 0], xzin[r, 1, 1])
        for m in range(M + 2):
            U[0, m] = swapped(C[m])
        small = (M, LANES)
        spot = iota(small, 1) % 4
        ends = (iota(small, 1) == 0) | (iota(small, 1) == LANES - 1)
        low_corner = jnp.where(spot == 1, yzin[r, 0, 0], yzin[r, 0, 1])
        high_corner = jnp.where(spot == 1, yzin[r, 1, 0], yzin[r, 1, 1])
        Y[0] = turn(low_corner, -4 * (T - 1))
        Y[1] = turn(high_corner, 4 * (T - 1))
        Y[2] = jnp.where(ends, turn(swapped(low_corner), LANES - 2 - 4 * (T - 1)), 0.0)
        Y[3] = jnp.where(ends, turn(swapped(high_corner), LANES - 2), 0.0)
        for m in range(M):
            a, b = zin[r, 0, m % H], zin[r, 1, m % H]
            if m >= H:
                a, b = turn(a, -2), turn(b, 2)
            mine = own[r, m]
            centre = C[m + 1]
            across = turn(jnp.where(place == 0, a, mine), 1) + turn(jnp.where(place == 3, b, mine), -1)
            above = turn(centre, -1, 0)
            above = jnp.where(sub == 7, turn(above, -4), above)
            above = jnp.where((sub == 7) & (group == T - 1), Y[1, m:m + 1], above)
            below = turn(centre, 1, 0)
            below = jnp.where(sub == 0, turn(below, 4), below)
            below = jnp.where((sub == 0) & (group == 0), Y[0, m:m + 1], below)
            near = jnp.where(odd8, C[m + 2], C[m])
            red = (SC[m] + centre + near + (across + (above + below))) * f32(SIXTH)
            U[1, m] = swapped(red)
        for m in range(M):
            for tiles in chunks:
                begin = PAD + 8 * tiles[0]
                value = update(h, m, begin, 8 * len(tiles), wings_of(U[0, m + 1], tiles))
                X[h + 1, m + 1, pl.ds(begin, 8 * len(tiles))] = value
            for k, begin in enumerate((PAD - 8, PAD + N)):
                X[h + 1, m + 1, pl.ds(begin, 8)] = update(
                    h, m, begin, 8, jnp.broadcast_to(Y[2 + k, m:m + 1], (8, LANES)))
        for k, (m, near) in enumerate(((-1, 0), (M, M - 1))):
            @pl.when(has[k])
            def _(m=m, near=near):
                for tiles in chunks:
                    begin = PAD + 8 * tiles[0]
                    X[h + 1, m + 1, pl.ds(begin, 8 * len(tiles))] = update(
                        h, m, begin, 8 * len(tiles), wings_of(U[0, m + 1], tiles), near)
        h += 1
        for number, m in enumerate(order):
            acc = jnp.zeros((8, LANES), f32)
            for tiles in chunks:
                begin, length = PAD + 8 * tiles[0], 8 * len(tiles)
                value = update(h, m, begin, length, wings_of(U[1, m], tiles))
                if r < SWEEPS - 1:
                    X[h + 1, m + 1, pl.ds(begin, length)] = value
                    for t in tiles:
                        acc = pack(acc, t, value[8 * (t - tiles[0]):8 * (t - tiles[0]) + 8])
                else:
                    red = X[h, m + 1, pl.ds(begin, length)]
                    obuf[2 * m, pl.ds(begin - PAD, length)] = jnp.where(odd_rows[:length], value, red)
                    obuf[2 * m + 1, pl.ds(begin - PAD, length)] = jnp.where(odd_rows[:length], red, value)
            if r < SWEEPS - 1:
                own[r + 1, m] = acc
                if number == 1:
                    start(r + 1, x_routes)
            else:
                pltpu.make_async_copy(obuf.at[pl.ds(2 * m, 2)], out.at[pl.ds(2 * m, 2)], osem.at[m]).start()
        if r < SWEEPS - 1:
            finish_pack(r + 1)
            start(r + 1, other_routes)

    for r in range(SWEEPS):
        for route in ROUTES:
            guarded(route[0], lambda route=route: remote(r, route).wait_send())
    for route in faces:
        guarded(route[0], lambda route=route: remote(SWEEPS, route).wait_send())
    for m in range(M):
        pltpu.make_async_copy(obuf.at[pl.ds(2 * m, 2)], out.at[pl.ds(2 * m, 2)], osem.at[m]).wait()


def on_device(field, source):
    L, N, K = field.shape
    M = L // 2
    vmem = lambda *shape: pltpu.VMEM(shape, f32)
    return pl.pallas_call(
        kernel,
        out_shape=jax.ShapeDtypeStruct(field.shape, f32),
        in_specs=[pl.BlockSpec(memory_space=pl.ANY)] * 2,
        out_specs=pl.BlockSpec(memory_space=pl.ANY),
        scratch_shapes=[
            vmem(L, N, K), vmem(L, N, K), vmem(L, N, K),
            vmem(2, M + 2, N + 2 * PAD, K),
            vmem(HALF, M + 2, N + 2 * PAD, K),
            vmem(SWEEPS, M, 8, K),
            vmem(SWEEPS, 2, M // 2, 8, K),
            vmem(SWEEPS, 2, M // 2, 8, K),
            vmem(SWEEPS, 2, 2, 8, K),
            vmem(SWEEPS, 2, M, K),
            vmem(SWEEPS, 2, 2, M, K),
            vmem(M, 8, K),
            vmem(2, M, 8, K),
            vmem(M, 8, K),
            vmem(M + 2, 8, K),
            vmem(2, M + 2, 8, K),
            vmem(4, M, K),
            pltpu.SemaphoreType.DMA((2, 4)),
            pltpu.SemaphoreType.DMA((M,)),
            pltpu.SemaphoreType.DMA((SWEEPS + 1, len(ROUTES))),
            pltpu.SemaphoreType.DMA((SWEEPS + 1, len(ROUTES))),
        ],
        compiler_params=pltpu.CompilerParams(collective_id=0, has_side_effects=True),
    )(field, source)


def solution(mesh):
    spec = P("gx", "gy", "gz")
    return jax.shard_map(on_device, mesh=mesh, in_specs=(spec, spec), out_specs=spec, check_vma=False)
```

```python
import functools
import itertools

import jax
import jax.numpy as jnp
from jax import lax
from jax.experimental import pallas as pl
from jax.experimental.pallas import tpu as pltpu
from jax.sharding import PartitionSpec as P

SWEEPS = 3
HALF = 2 * SWEEPS
PAD = 16
LANES = 128
CHUNK = 8
SIXTH = 1.0 / 6.0
MESH = pl.DeviceIdType.MESH
AXES = ("gx", "gy", "gz")
ROUTES = [r for r in itertools.product((-1, 0, 1), repeat=3) if 1 <= sum(map(abs, r)) <= 2]
f32 = jnp.float32
bf16 = jnp.bfloat16


def iota(shape, dim):
    return lax.broadcasted_iota(jnp.int32, shape, dim)


def side(step):
    return 0 if step < 0 else 1


def kernel(field, source, obuf, fbuf, sbuf, S, X, own, zout, zin, xzin, yzout, yzin,
           sown, szin, sxout, sxin, SC, C, U, Y, isem, ssem, rsem):
    M = X.shape[1] - 2
    N = X.shape[2] - 2 * PAD
    T = N // 8
    H = M // 2
    at = {a: lax.axis_index(a) for a in AXES}
    size = {a: lax.axis_size(a) for a in AXES}
    has = (at["gx"] > 0, at["gx"] < size["gx"] - 1)

    def target(route):
        return {a: lax.rem(at[a] + step + size[a], size[a]) for a, step in zip(AXES, route) if step}

    def guarded(step, action):
        if step == 0:
            action()
        else:
            pl.when(has[side(step)])(action)

    rows = pl.ds(PAD, N)
    inner = pl.ds(1, M)
    first, last = pl.ds(PAD, 8), pl.ds(PAD + N - 8, 8)
    before, after = pl.ds(PAD - 8, 8), pl.ds(PAD + N, 8)
    edge_rows = ((first, after), (last, before))

    def refs(r, route):
        x, y, z = route
        h = 2 * r
        if x:
            src_plane, dst_plane = ((1, M + 1), (M, 0))[side(x)]
        if y:
            src_rows, dst_rows = edge_rows[side(y)]
        if x and y:
            return X.at[h, src_plane, src_rows], X.at[h, dst_plane, dst_rows]
        if x and z:
            return own.at[r, src_plane - 1], xzin.at[r, side(-x), side(-z)]
        if y and z:
            return yzout.at[r, side(y)], yzin.at[r, side(-y), side(-z)]
        if x:
            return X.at[h, src_plane, rows], X.at[h, dst_plane, rows]
        if y:
            return X.at[h, inner, src_rows], X.at[h, inner, dst_rows]
        return zout.at[r, side(z)], zin.at[r, side(-z)]

    def source_refs(route):
        x, y, z = route
        if x:
            return sxout.at[side(x)], sxin.at[side(-x)]
        if y:
            src_rows, dst_rows = edge_rows[side(y)]
            return S.at[0, inner, src_rows], S.at[0, inner, dst_rows]
        return sown, szin.at[side(-z)]

    def remote(r, route):
        pair = refs(r, route) if r < SWEEPS else source_refs(route)
        number = ROUTES.index(route)
        return pltpu.make_async_remote_copy(
            src_ref=pair[0], dst_ref=pair[1], send_sem=ssem.at[r, number], recv_sem=rsem.at[r, number],
            device_id=target(route), device_id_type=MESH)

    faces = [r for r in ROUTES if sum(map(abs, r)) == 1]
    edges = [r for r in ROUTES if sum(map(abs, r)) == 2]
    edges.sort(key=lambda r: abs(r[0]))
    x_faces = [r for r in faces if r[0]]
    yz_faces = [r for a in (2, 1) for r in faces if r[a]]
    yz_edges = [r for r in edges if not r[0]]
    early = [r for r in edges if r[0]] + yz_faces
    ordered = edges + yz_faces + x_faces

    def start(r, routes):
        for route in routes:
            guarded(route[0], lambda route=route: remote(r, route).start())

    def wait(r, routes):
        for route in routes:
            guarded(-route[0], lambda route=route: remote(r, route).wait_recv())

    planes = 2 * M // 4
    loads = []
    for slot, (big, small) in enumerate(((field, fbuf), (source, sbuf))):
        for part in (0, 3, 1, 2):
            here = pl.ds(part * planes, planes)
            loads.append(pltpu.make_async_copy(big.at[here], small.at[here], isem.at[slot, part]))
    for load in loads:
        load.start()
    barrier = pltpu.get_barrier_semaphore()
    count = jnp.int32(0)
    for route in ROUTES:
        guarded(route[0], lambda route=route: pl.semaphore_signal(
            barrier, inc=1, device_id=target(route), device_id_type=MESH))
        count = count + (1 if route[0] == 0 else has[side(route[0])].astype(jnp.int32))

    lane = iota((8, LANES), 1)
    sub = iota((8, LANES), 0)
    group = lane // 4
    place = lane % 4
    odd8 = (sub + lane) % 2 == 1
    outer = (lane == 0) | (lane == LANES - 1)
    odd_rows = (iota((8 * CHUNK, LANES), 0) + iota((8 * CHUNK, LANES), 1)) % 2 == 1
    outer_rows = (iota((8 * CHUNK, LANES), 1) == 0) | (iota((8 * CHUNK, LANES), 1) == LANES - 1)
    row_of = iota((8 * CHUNK, LANES), 0)
    gap = jnp.abs(iota((LANES, LANES), 0) - iota((LANES, LANES), 1))
    beside_lanes = jnp.where(gap == 1, 1.0, 0.0).astype(bf16)
    beside_lanes = jnp.concatenate([beside_lanes, beside_lanes], 0)

    def turn(value, shift, axis=1):
        return pltpu.roll(value, shift % value.shape[axis], axis)

    def lane_sum(value):
        high = value.astype(bf16)
        rest = (value - high.astype(f32)).astype(bf16)
        return jnp.dot(jnp.concatenate([high, rest], 1), beside_lanes, preferred_element_type=f32)

    def swapped(value):
        where = iota(value.shape, 1) % 4
        return jnp.where(where == 1, turn(value, -1), turn(value, 1))

    def pack(acc, t, tile):
        return jnp.where(group == t, turn(tile, 4 * t + 2), acc)

    @pl.when(at["gx"] == 0)
    def _():
        for h in range(HALF):
            X[h, 0] = jnp.zeros(X.shape[2:], f32)
        for r in range(SWEEPS):
            xzin[r, 0] = jnp.zeros(xzin.shape[2:], f32)

    @pl.when(at["gx"] == size["gx"] - 1)
    def _():
        for h in range(HALF):
            X[h, M + 1] = jnp.zeros(X.shape[2:], f32)
        for r in range(SWEEPS):
            xzin[r, 1] = jnp.zeros(xzin.shape[2:], f32)

    def finish_pack(r):
        for m in range(H):
            one, two = own[r, m], own[r, m + H]
            zout[r, 0, m] = jnp.where(place >= 2, one, turn(two, -2))
            zout[r, 1, m] = jnp.where(place < 2, one, turn(two, 2))
        for m in range(M):
            yzout[r, 0, m:m + 1] = own[r, m, 0:1]
            yzout[r, 1, m:m + 1] = own[r, m, 7:8]

    order = [0, M - 1] + list(range(1, M - 1))
    whole_odd = (iota((N, LANES), 0) + iota((N, LANES), 1)) % 2 == 1

    for load in loads[:4]:
        load.wait()
    for m in order:
        value = jnp.where(whole_odd, fbuf[2 * m], fbuf[2 * m + 1])
        X[0, m + 1, rows] = value
        acc = jnp.zeros((8, LANES), f32)
        for t in range(T):
            acc = pack(acc, t, value[8 * t:8 * t + 8])
        own[0, m] = acc
    finish_pack(0)
    pl.semaphore_wait(barrier, count)
    start(0, ordered)

    for load in loads[4:]:
        load.wait()
    for m in order:
        even_plane, odd_plane = sbuf[2 * m], sbuf[2 * m + 1]
        value = jnp.where(whole_odd, odd_plane, even_plane)
        S[0, m + 1, rows] = value
        S[1, m + 1, rows] = jnp.where(whole_odd, even_plane, odd_plane)
        acc = jnp.zeros((8, LANES), f32)
        for t in (range(T)):
            acc = pack(acc, t, value[8 * t:8 * t + 8])
        sown[m] = acc
        if m in (0, M - 1):
            top, bottom = value[:N // 2], pltpu.roll(value[N // 2:], 1, 1)
            odd_half = whole_odd[:N // 2]
            if m == 0:
                sxout[0] = jnp.where(odd_half, bottom, top)
            if m == M - 1:
                sxout[1] = jnp.where(odd_half, top, bottom)
    start(SWEEPS, yz_faces + x_faces)

    def update(h, m, start_row, length, wings, near=None):
        here = pl.ds(start_row, length)
        centre = X[h, m + 1, here]
        if near is None:
            low, high = X[h, m, here], X[h, m + 2, here]
            if h % 2:
                low, high = high, low
            near = jnp.where(odd_rows[:length], high, low)
        else:
            near = X[h, near + 1, here]
        total = (S[h % 2, m + 1, here] + centre) + (near + lane_sum(centre))
        total = total + (X[h, m + 1, pl.ds(start_row - 1, length)] + X[h, m + 1, pl.ds(start_row + 1, length)])
        if wings is not None:
            total = total + jnp.where(outer_rows[:length], wings, 0.0)
        return total * f32(SIXTH)

    def wings_of(edge, tiles):
        return jnp.concatenate([turn(edge, LANES - 2 - 4 * t) for t in tiles], 0)

    chunks = [range(c, min(c + CHUNK, T)) for c in range(0, T, CHUNK)]

    for r in range(SWEEPS):
        h = 2 * r
        wait(r, early)
        if r == 0:
            wait(SWEEPS, yz_faces)
            for m in range(M):
                SC[m] = jnp.where(place == 1, szin[0, m], szin[1, m])
        for m in range(M):
            a, b = zin[r, 0, m % H], zin[r, 1, m % H]
            if m >= H:
                a, b = turn(a, -2), turn(b, 2)
            C[m + 1] = jnp.where(place == 1, a, b)
        C[0] = jnp.where(place == 1, xzin[r, 0, 0], xzin[r, 0, 1])
        C[M + 1] = jnp.where(place == 1, xzin[r, 1, 0], xzin[r, 1, 1])
        for m in range(M + 2):
            U[0, m] = swapped(C[m])
        for m in range(M):
            a, b = zin[r, 0, m % H], zin[r, 1, m % H]
            if m >= H:
                a, b = turn(a, -2), turn(b, 2)
            mine = own[r, m]
            centre = C[m + 1]
            across = turn(jnp.where(place == 0, a, mine), 1) + turn(jnp.where(place == 3, b, mine), -1)
            above = turn(centre, -1, 0)
            above = jnp.where(sub == 7, turn(above, -4), above)
            above = jnp.where((sub == 7) & (group == T - 1), 0.0, above)
            below = turn(centre, 1, 0)
            below = jnp.where(sub == 0, turn(below, 4), below)
            below = jnp.where((sub == 0) & (group == 0), 0.0, below)
            near = jnp.where(odd8, C[m + 2], C[m])
            red = (SC[m] + centre + near + (across + (above + below))) * f32(SIXTH)
            U[1, m] = swapped(red)
        def red_plane(m, near=None):
            for tiles in chunks:
                begin = PAD + 8 * tiles[0]
                X[h + 1, m + 1, pl.ds(begin, 8 * len(tiles))] = update(
                    h, m, begin, 8 * len(tiles), wings_of(U[0, m + 1], tiles), near)

        for m in range(1, M - 1):
            red_plane(m)
        for m in range(M):
            for begin in (PAD - 8, PAD + N):
                X[h + 1, m + 1, pl.ds(begin, 8)] = update(h, m, begin, 8, None)
        wait(r, x_faces)
        if r == 0:
            wait(SWEEPS, x_faces)
            for k, plane in enumerate((0, M + 1)):
                @pl.when(has[k])
                def _(k=k, plane=plane):
                    half = sxin[k]
                    S[0, plane, pl.ds(PAD, N // 2)] = half
                    S[0, plane, pl.ds(PAD + N // 2, N // 2)] = pltpu.roll(half, LANES - 1, 1)
        for k, (m, near) in enumerate(((-1, 0), (M, M - 1))):
            pl.when(has[k])(functools.partial(red_plane, m, near))
        red_plane(0)
        red_plane(M - 1)
        wait(r, yz_edges)
        small = (M, LANES)
        spot = iota(small, 1) % 4
        ends = (iota(small, 1) == 0) | (iota(small, 1) == LANES - 1)
        low_corner = jnp.where(spot == 1, yzin[r, 0, 0], yzin[r, 0, 1])
        high_corner = jnp.where(spot == 1, yzin[r, 1, 0], yzin[r, 1, 1])
        Y[0] = jnp.where(ends, turn(swapped(low_corner), LANES - 2 - 4 * (T - 1)), 0.0) * f32(1.0 / 18.0)
        Y[1] = jnp.where(ends, turn(swapped(high_corner), LANES - 2), 0.0) * f32(1.0 / 18.0)
        h += 1
        for number, m in enumerate(order):
            acc = jnp.zeros((8, LANES), f32)
            for tiles in chunks:
                begin, length = PAD + 8 * tiles[0], 8 * len(tiles)
                value = update(h, m, begin, length, wings_of(U[1, m], tiles))
                if tiles[0] == 0:
                    value = value + jnp.where(row_of[:length] == 0, Y[0, m:m + 1], 0.0)
                if tiles[-1] == T - 1:
                    value = value + jnp.where(row_of[:length] == length - 1, Y[1, m:m + 1], 0.0)
                if r < SWEEPS - 1:
                    X[h + 1, m + 1, pl.ds(begin, length)] = value
                    for t in tiles:
                        acc = pack(acc, t, value[8 * (t - tiles[0]):8 * (t - tiles[0]) + 8])
                else:
                    red = X[h, m + 1, pl.ds(begin, length)]
                    obuf[2 * m, pl.ds(begin - PAD, length)] = jnp.where(odd_rows[:length], value, red)
                    obuf[2 * m + 1, pl.ds(begin - PAD, length)] = jnp.where(odd_rows[:length], red, value)
            if r < SWEEPS - 1:
                own[r + 1, m] = acc
        if r < SWEEPS - 1:
            finish_pack(r + 1)
            start(r + 1, ordered)

    for r in range(SWEEPS):
        for route in ROUTES:
            guarded(route[0], lambda route=route: remote(r, route).wait_send())
    for route in faces:
        guarded(route[0], lambda route=route: remote(SWEEPS, route).wait_send())


def on_device(field, source):
    L, N, K = field.shape
    M = L // 2
    vmem = lambda *shape: pltpu.VMEM(shape, f32)
    return pl.pallas_call(
        kernel,
        out_shape=jax.ShapeDtypeStruct(field.shape, f32),
        in_specs=[pl.BlockSpec(memory_space=pltpu.HBM)] * 2,
        out_specs=pl.BlockSpec(memory_space=pltpu.VMEM),
        scratch_shapes=[
            vmem(L, N, K), vmem(L, N, K),
            vmem(2, M + 2, N + 2 * PAD, K),
            vmem(HALF, M + 2, N + 2 * PAD, K),
            vmem(SWEEPS, M, 8, K),
            vmem(SWEEPS, 2, M // 2, 8, K),
            vmem(SWEEPS, 2, M // 2, 8, K),
            vmem(SWEEPS, 2, 2, 8, K),
            vmem(SWEEPS, 2, M, K),
            vmem(SWEEPS, 2, 2, M, K),
            vmem(M, 8, K),
            vmem(2, M, 8, K),
            vmem(2, N // 2, K), vmem(2, N // 2, K),
            vmem(M, 8, K),
            vmem(M + 2, 8, K),
            vmem(2, M + 2, 8, K),
            vmem(2, M, K),
            pltpu.SemaphoreType.DMA((2, 4)),
            pltpu.SemaphoreType.DMA((SWEEPS + 1, len(ROUTES))),
            pltpu.SemaphoreType.DMA((SWEEPS + 1, len(ROUTES))),
        ],
        compiler_params=pltpu.CompilerParams(collective_id=0, has_side_effects=True, vmem_limit_bytes=40 << 20),
    )(pltpu.with_memory_space_constraint(field, pltpu.HBM), pltpu.with_memory_space_constraint(source, pltpu.HBM))


def solution(mesh):
    spec = P("gx", "gy", "gz")
    return jax.shard_map(on_device, mesh=mesh, in_specs=(spec, spec), out_specs=spec, check_vma=False)
```

```python
import functools
import itertools

import jax
import jax.numpy as jnp
from jax import lax
from jax.experimental import pallas as pl
from jax.experimental.pallas import tpu as pltpu
from jax.sharding import PartitionSpec as P

SWEEPS = 3
HALF = 2 * SWEEPS
PAD = 16
LANES = 128
CHUNK = 8
SIXTH = 1.0 / 6.0
MESH = pl.DeviceIdType.MESH
AXES = ("gx", "gy", "gz")
ROUTES = [r for r in itertools.product((-1, 0, 1), repeat=3) if 1 <= sum(map(abs, r)) <= 2]
f32 = jnp.float32
bf16 = jnp.bfloat16


def iota(shape, dim):
    return lax.broadcasted_iota(jnp.int32, shape, dim)


def side(step):
    return 0 if step < 0 else 1


def kernel(field, source, obuf, fbuf, sbuf, S, X, own, zout, zin, xzin, yzout, yzin,
           sown, szin, sxout, sxin, SC, C, U, Y, SZ, V, DZ, PK, DY, DYR, DR, DX, isem, ssem, rsem):
    M = X.shape[1] - 2
    N = X.shape[2] - 2 * PAD
    T = N // 8
    H = M // 2
    at = {a: lax.axis_index(a) for a in AXES}
    size = {a: lax.axis_size(a) for a in AXES}
    has = (at["gx"] > 0, at["gx"] < size["gx"] - 1)

    def target(route):
        return {a: lax.rem(at[a] + step + size[a], size[a]) for a, step in zip(AXES, route) if step}

    def guarded(step, action):
        if step == 0:
            action()
        else:
            pl.when(has[side(step)])(action)

    rows = pl.ds(PAD, N)
    inner = pl.ds(1, M)
    first, last = pl.ds(PAD, 8), pl.ds(PAD + N - 8, 8)
    before, after = pl.ds(PAD - 8, 8), pl.ds(PAD + N, 8)
    edge_rows = ((first, after), (last, before))

    def refs(r, route):
        x, y, z = route
        h = 2 * r
        if x:
            src_plane, dst_plane = ((1, M + 1), (M, 0))[side(x)]
        if y:
            src_rows, dst_rows = edge_rows[side(y)]
        if x and y:
            return X.at[h, src_plane, src_rows], X.at[h, dst_plane, dst_rows]
        if x and z:
            return own.at[r, src_plane - 1], xzin.at[r, side(-x), side(-z)]
        if y and z:
            return yzout.at[r, side(y)], yzin.at[r, side(-y), side(-z)]
        if x:
            return X.at[h, src_plane, rows], X.at[h, dst_plane, rows]
        if y:
            return X.at[h, inner, src_rows], X.at[h, inner, dst_rows]
        return zout.at[r, side(z)], zin.at[r, side(-z)]

    def source_refs(route):
        x, y, z = route
        if x:
            return sxout.at[side(x)], sxin.at[side(-x)]
        if y:
            src_rows, dst_rows = edge_rows[side(y)]
            return S.at[0, inner, src_rows], S.at[0, inner, dst_rows]
        return sown, szin.at[side(-z)]

    def remote(r, route):
        pair = refs(r, route) if r < SWEEPS else source_refs(route)
        number = ROUTES.index(route)
        return pltpu.make_async_remote_copy(
            src_ref=pair[0], dst_ref=pair[1], send_sem=ssem.at[r, number], recv_sem=rsem.at[r, number],
            device_id=target(route), device_id_type=MESH)

    faces = [r for r in ROUTES if sum(map(abs, r)) == 1]
    edges = [r for r in ROUTES if sum(map(abs, r)) == 2]
    edges.sort(key=lambda r: abs(r[0]))
    x_faces = [r for r in faces if r[0]]
    yz_faces = [r for a in (2, 1) for r in faces if r[a]]
    yz_edges = [r for r in edges if not r[0]]
    early = [r for r in edges if r[0]] + yz_faces
    ordered = edges + yz_faces + x_faces

    def start(r, routes):
        for route in routes:
            guarded(route[0], lambda route=route: remote(r, route).start())

    def wait(r, routes):
        for route in routes:
            guarded(-route[0], lambda route=route: remote(r, route).wait_recv())

    planes = 2 * M // 4
    loads = []
    for slot, (big, small) in enumerate(((field, fbuf), (source, sbuf))):
        for part in (0, 3, 1, 2):
            here = pl.ds(part * planes, planes)
            loads.append(pltpu.make_async_copy(big.at[here], small.at[here], isem.at[slot, part]))
    for load in loads:
        load.start()
    barrier = pltpu.get_barrier_semaphore()
    count = jnp.int32(0)
    for route in ROUTES:
        guarded(route[0], lambda route=route: pl.semaphore_signal(
            barrier, inc=1, device_id=target(route), device_id_type=MESH))
        count = count + (1 if route[0] == 0 else has[side(route[0])].astype(jnp.int32))

    lane = iota((8, LANES), 1)
    sub = iota((8, LANES), 0)
    group = lane // 4
    place = lane % 4
    odd8 = (sub + lane) % 2 == 1
    outer = (lane == 0) | (lane == LANES - 1)
    odd_rows = (iota((8 * CHUNK, LANES), 0) + iota((8 * CHUNK, LANES), 1)) % 2 == 1
    outer_rows = (iota((8 * CHUNK, LANES), 1) == 0) | (iota((8 * CHUNK, LANES), 1) == LANES - 1)
    row_of = iota((8 * CHUNK, LANES), 0)
    rim_rows = (iota((8 * CHUNK, LANES), 1) < 2) | (iota((8 * CHUNK, LANES), 1) >= LANES - 2)
    gap = jnp.abs(iota((LANES, LANES), 0) - iota((LANES, LANES), 1))
    beside_lanes = jnp.where(gap == 1, 1.0, 0.0).astype(bf16)
    beside_lanes = jnp.concatenate([beside_lanes, beside_lanes], 0)

    def turn(value, shift, axis=1):
        return pltpu.roll(value, shift % value.shape[axis], axis)

    def lane_sum(value):
        high = value.astype(bf16)
        rest = (value - high.astype(f32)).astype(bf16)
        return jnp.dot(jnp.concatenate([high, rest], 1), beside_lanes, preferred_element_type=f32)

    def swapped(value):
        where = iota(value.shape, 1) % 4
        return jnp.where(where == 1, turn(value, -1), turn(value, 1))

    def pack(acc, t, tile):
        return jnp.where(group == t, turn(tile, 4 * t + 2), acc)

    @pl.when(at["gx"] == 0)
    def _():
        for h in range(HALF):
            X[h, 0] = jnp.zeros(X.shape[2:], f32)
        for r in range(SWEEPS):
            xzin[r, 0] = jnp.zeros(xzin.shape[2:], f32)

    @pl.when(at["gx"] == size["gx"] - 1)
    def _():
        for h in range(HALF):
            X[h, M + 1] = jnp.zeros(X.shape[2:], f32)
        for r in range(SWEEPS):
            xzin[r, 1] = jnp.zeros(xzin.shape[2:], f32)

    def finish_pack(r):
        for m in range(H):
            one, two = own[r, m], own[r, m + H]
            zout[r, 0, m] = jnp.where(place >= 2, one, turn(two, -2))
            zout[r, 1, m] = jnp.where(place < 2, one, turn(two, 2))
        for m in range(M):
            yzout[r, 0, m:m + 1] = own[r, m, 0:1]
            yzout[r, 1, m:m + 1] = own[r, m, 7:8]

    V[0] = jnp.zeros((8, LANES), f32)
    V[M + 1] = jnp.zeros((8, LANES), f32)
    for k in range(2):
        DR[k, 0:8] = jnp.zeros((8, LANES), f32)
        DR[k, N + 8:N + 16] = jnp.zeros((8, LANES), f32)
    order = [0, M - 1] + list(range(1, M - 1))
    whole_odd = (iota((N, LANES), 0) + iota((N, LANES), 1)) % 2 == 1

    for load in loads[:4]:
        load.wait()
    for m in order:
        value = jnp.where(whole_odd, fbuf[2 * m], fbuf[2 * m + 1])
        X[0, m + 1, rows] = value
        acc = jnp.zeros((8, LANES), f32)
        for t in range(T):
            acc = pack(acc, t, value[8 * t:8 * t + 8])
        own[0, m] = acc
    finish_pack(0)
    pl.semaphore_wait(barrier, count)
    start(0, ordered)

    for load in loads[4:]:
        load.wait()
    for m in order:
        even_plane, odd_plane = sbuf[2 * m], sbuf[2 * m + 1]
        value = jnp.where(whole_odd, odd_plane, even_plane)
        S[0, m + 1, rows] = value
        S[1, m + 1, rows] = jnp.where(whole_odd, even_plane, odd_plane)
        acc = jnp.zeros((8, LANES), f32)
        for t in (range(T)):
            acc = pack(acc, t, value[8 * t:8 * t + 8])
        sown[m] = acc
        if m in (0, M - 1):
            top, bottom = value[:N // 2], pltpu.roll(value[N // 2:], 1, 1)
            odd_half = whole_odd[:N // 2]
            if m == 0:
                sxout[0] = jnp.where(odd_half, bottom, top)
            if m == M - 1:
                sxout[1] = jnp.where(odd_half, top, bottom)
    start(SWEEPS, yz_faces + x_faces)

    def update(h, m, start_row, length, wings, near=None):
        here = pl.ds(start_row, length)
        centre = X[h, m + 1, here]
        if near is None:
            near = jnp.where(odd_rows[:length], X[h, m + 2, here], X[h, m, here])
        else:
            near = X[h, near + 1, here]
        total = (S[0, m + 1, here] + centre) + (near + lane_sum(centre))
        total = total + (X[h, m + 1, pl.ds(start_row - 1, length)] + X[h, m + 1, pl.ds(start_row + 1, length)])
        if wings is not None:
            total = total + jnp.where(outer_rows[:length], wings, 0.0)
        return total * f32(SIXTH)

    def inside(h, m, tiles):
        start_row, length = PAD + 8 * tiles[0], 8 * len(tiles)
        here = pl.ds(start_row, length)
        centre = X[h, m + 1, here]
        low = X[h, m, here] if m > 0 else 0.0
        high = X[h, m + 2, here] if m < M - 1 else 0.0
        if h % 2:
            low, high = high, low
        total = (S[h % 2, m + 1, here] + centre) + (jnp.where(odd_rows[:length], high, low) + lane_sum(centre))
        if tiles[0] == 0:
            down = jnp.where(row_of[:length] == 0, 0.0, pltpu.roll(centre, 1, 0))
        else:
            down = X[h, m + 1, pl.ds(start_row - 1, length)]
        if tiles[-1] == T - 1:
            above = jnp.where(row_of[:length] == length - 1, 0.0, pltpu.roll(centre, length - 1, 0))
        else:
            above = X[h, m + 1, pl.ds(start_row + 1, length)]
        return (total + (down + above)) * f32(SIXTH)

    def wings_of(edge, tiles):
        return jnp.concatenate([turn(edge, LANES - 2 - 4 * t) for t in tiles], 0)

    def spread(edge, tiles):
        return jnp.where(rim_rows[:8 * len(tiles)], wings_of(edge, tiles), 0.0)

    def shifted(value):
        above = turn(value, -1, 0)
        above = jnp.where(sub == 7, turn(above, -4), above)
        above = jnp.where((sub == 7) & (group == T - 1), 0.0, above)
        below = turn(value, 1, 0)
        below = jnp.where(sub == 0, turn(below, 4), below)
        below = jnp.where((sub == 0) & (group == 0), 0.0, below)
        return above + below

    chunks = [range(c, min(c + CHUNK, T)) for c in range(0, T, CHUNK)]
    middle = (place == 1) | (place == 2)
    zero8 = jnp.zeros((8, LANES), f32)

    def padded(tiles, low, high):
        parts = [zero8] * len(tiles)
        if tiles[0] == 0:
            parts[0] = low
        if tiles[-1] == T - 1:
            parts[-1] = high
        return jnp.concatenate(parts, 0) if tiles[0] == 0 or tiles[-1] == T - 1 else None

    for r in range(SWEEPS):
        h = 2 * r
        ended = r == SWEEPS - 1
        if r > 0:
            for m in range(1, M - 1):
                for tiles in chunks:
                    tiles = [t for t in tiles if 0 < t < T - 1]
                    here = pl.ds(PAD + 8 * tiles[0], 8 * len(tiles))
                    X[h, m + 1, here] = X[h, m + 1, here] + spread(DZ[m], tiles)
        for m in range(M):
            for tiles in chunks:
                X[h + 1, m + 1, pl.ds(PAD + 8 * tiles[0], 8 * len(tiles))] = inside(h, m, tiles)
        for m in range(M):
            acc = zero8
            for tiles in chunks:
                value = inside(h + 1, m, tiles)
                X[h + 2, m + 1, pl.ds(PAD + 8 * tiles[0], 8 * len(tiles))] = value
                if not ended and 0 < m < M - 1:
                    for t in tiles:
                        acc = pack(acc, t, value[8 * (t - tiles[0]):8 * (t - tiles[0]) + 8])
            PK[m] = acc

        wait(r, early)
        if r == 0:
            wait(SWEEPS, yz_faces)
            for m in range(M):
                SC[m] = jnp.where(place == 1, szin[0, m], szin[1, m])
        for m in range(M):
            a, b = zin[r, 0, m % H], zin[r, 1, m % H]
            if m >= H:
                a, b = turn(a, -2), turn(b, 2)
            mine = own[r, m]
            C[m + 1] = jnp.where(place == 1, a, b)
            SZ[m] = turn(jnp.where(place == 0, a, mine), 1) + turn(jnp.where(place == 3, b, mine), -1)
        C[0] = jnp.where(place == 1, xzin[r, 0, 0], xzin[r, 0, 1])
        C[M + 1] = jnp.where(place == 1, xzin[r, 1, 0], xzin[r, 1, 1])
        U[0] = swapped(C[0])
        U[1] = swapped(C[M + 1])
        for m in range(M):
            V[m + 1] = jnp.where(middle, swapped(C[m + 1]), 0.0) * f32(SIXTH)
        for m in range(M):
            centre = C[m + 1]
            near = jnp.where(odd8, C[m + 2], C[m])
            red = (SC[m] + centre + near + (SZ[m] + shifted(centre))) * f32(SIXTH)
            mine = V[m + 1]
            near = jnp.where(odd8, V[m], V[m + 2])
            total = (swapped(red) + mine) + (near + shifted(mine))
            DZ[m] = jnp.where(middle, total, jnp.where(place == 0, turn(mine, -1), turn(mine, 1))) * f32(SIXTH)
        for k, (begin, row, end, following) in enumerate(((PAD - 8, PAD - 1, 0, 1), (PAD + N, PAD + N, 7, 6))):
            for m in range(M):
                X[h + 1, m + 1, pl.ds(begin, 8)] = update(h, m, begin, 8, None)
            change = [jnp.broadcast_to(X[h, m + 1, row:row + 1], (8, LANES)) * f32(SIXTH) for m in range(M)]
            sums = lane_sum(jnp.concatenate(change, 0))
            for m in range(M):
                low = change[m - 1] if m > 0 else 0.0
                high = change[m + 1] if m < M - 1 else 0.0
                near = jnp.where(lane % 2 == 1 - k, low, high)
                total = (X[h + 1, m + 1, row:row + 1] + change[m]) + (near + sums[8 * m:8 * m + 8])
                DY[k, m] = jnp.where(sub == end, total, jnp.where(sub == following, change[m], 0.0)) * f32(SIXTH)
                if ended:
                    DYR[k, m] = jnp.where(sub == end, change[m], 0.0)
        wait(r, x_faces)
        if r == 0:
            wait(SWEEPS, x_faces)
            for k, plane in enumerate((0, M + 1)):
                half = sxin[k]
                S[0, plane, pl.ds(PAD, N // 2)] = half
                S[0, plane, pl.ds(PAD + N // 2, N // 2)] = pltpu.roll(half, LANES - 1, 1)
        for k, (m, near) in enumerate(((-1, 0), (M, M - 1))):
            for tiles in chunks:
                begin, length = PAD + 8 * tiles[0], 8 * len(tiles)
                odd = odd_rows[:length]
                red = update(h, m, begin, length, wings_of(U[k], tiles), near)
                bare = X[h, m + 1, pl.ds(begin, length)] * f32(SIXTH)
                if k == 0:
                    red, bare = jnp.where(odd, red, 0.0), jnp.where(odd, 0.0, bare)
                else:
                    red, bare = jnp.where(odd, 0.0, red), jnp.where(odd, bare, 0.0)
                DR[k, pl.ds(8 + 8 * tiles[0], length)] = bare
                DX[k, pl.ds(8 * tiles[0], length)] = jnp.where(has[k], red, 0.0) + (bare + lane_sum(bare))
            for tiles in chunks:
                begin, length = 8 * tiles[0], 8 * len(tiles)
                here = pl.ds(begin, length)
                DX[k, here] = (DX[k, here] + (DR[k, pl.ds(7 + begin, length)] + DR[k, pl.ds(9 + begin, length)])) * f32(SIXTH)
        wait(r, yz_edges)
        small = (M, LANES)
        spot = iota(small, 1) % 4
        ends = (iota(small, 1) == 0) | (iota(small, 1) == LANES - 1)
        low_corner = jnp.where(spot == 1, yzin[r, 0, 0], yzin[r, 0, 1])
        high_corner = jnp.where(spot == 1, yzin[r, 1, 0], yzin[r, 1, 1])
        Y[0] = jnp.where(ends, turn(swapped(low_corner), LANES - 2 - 4 * (T - 1)), 0.0) * f32(1.0 / 18.0)
        Y[1] = jnp.where(ends, turn(swapped(high_corner), LANES - 2), 0.0) * f32(1.0 / 18.0)
        for m in range(M):
            DY[0, m] = DY[0, m] + jnp.where(sub == 0, Y[0, m:m + 1], 0.0)
            DY[1, m] = DY[1, m] + jnp.where(sub == 7, Y[1, m:m + 1], 0.0)

        def black(m, tiles):
            value = X[h + 2, m + 1, pl.ds(PAD + 8 * tiles[0], 8 * len(tiles))] + spread(DZ[m], tiles)
            extra = padded(tiles, DY[0, m], DY[1, m])
            if extra is not None:
                value = value + extra
            if m in (0, M - 1):
                value = value + DX[0 if m == 0 else 1, pl.ds(8 * tiles[0], 8 * len(tiles))]
            return value

        if not ended:
            for m in (0, M - 1):
                acc = zero8
                for tiles in chunks:
                    value = black(m, tiles)
                    X[h + 2, m + 1, pl.ds(PAD + 8 * tiles[0], 8 * len(tiles))] = value
                    for t in tiles:
                        acc = pack(acc, t, value[8 * (t - tiles[0]):8 * (t - tiles[0]) + 8])
                own[r + 1, m] = acc
            start(r + 1, [q for q in edges if q[0]] + x_faces)
            for m in range(1, M - 1):
                for t in (0, T - 1):
                    X[h + 2, m + 1, pl.ds(PAD + 8 * t, 8)] = black(m, [t])
                low = jnp.where(group == 0, turn(DY[0, m], 2), 0.0)
                high = jnp.where(group == T - 1, turn(DY[1, m], 4 * T - 2), 0.0)
                own[r + 1, m] = (PK[m] + DZ[m]) + (low + high)
            finish_pack(r + 1)
            start(r + 1, [q for q in ordered if not q[0]])
        else:
            for m in range(M):
                for tiles in chunks:
                    begin, length = 8 * tiles[0], 8 * len(tiles)
                    value = black(m, tiles)
                    red = X[h + 1, m + 1, pl.ds(PAD + begin, length)] + spread(V[m + 1], tiles)
                    extra = padded(tiles, DYR[0, m], DYR[1, m])
                    if extra is not None:
                        red = red + extra
                    if m in (0, M - 1):
                        red = red + DR[0 if m == 0 else 1, pl.ds(8 + begin, length)]
                    obuf[2 * m, pl.ds(begin, length)] = jnp.where(odd_rows[:length], value, red)
                    obuf[2 * m + 1, pl.ds(begin, length)] = jnp.where(odd_rows[:length], red, value)

    for r in range(SWEEPS):
        for route in ROUTES:
            guarded(route[0], lambda route=route: remote(r, route).wait_send())
    for route in faces:
        guarded(route[0], lambda route=route: remote(SWEEPS, route).wait_send())


def on_device(field, source):
    L, N, K = field.shape
    M = L // 2
    vmem = lambda *shape: pltpu.VMEM(shape, f32)
    return pl.pallas_call(
        kernel,
        out_shape=jax.ShapeDtypeStruct(field.shape, f32),
        in_specs=[pl.BlockSpec(memory_space=pltpu.HBM)] * 2,
        out_specs=pl.BlockSpec(memory_space=pltpu.VMEM),
        scratch_shapes=[
            vmem(L, N, K), vmem(L, N, K),
            vmem(2, M + 2, N + 2 * PAD, K),
            vmem(HALF + 1, M + 2, N + 2 * PAD, K),
            vmem(SWEEPS, M, 8, K),
            vmem(SWEEPS, 2, M // 2, 8, K),
            vmem(SWEEPS, 2, M // 2, 8, K),
            vmem(SWEEPS, 2, 2, 8, K),
            vmem(SWEEPS, 2, M, K),
            vmem(SWEEPS, 2, 2, M, K),
            vmem(M, 8, K),
            vmem(2, M, 8, K),
            vmem(2, N // 2, K), vmem(2, N // 2, K),
            vmem(M, 8, K),
            vmem(M + 2, 8, K),
            vmem(2, 8, K),
            vmem(2, M, K),
            vmem(M, 8, K),
            vmem(M + 2, 8, K),
            vmem(M, 8, K),
            vmem(M, 8, K),
            vmem(2, M, 8, K),
            vmem(2, M, 8, K),
            vmem(2, N + 16, K),
            vmem(2, N, K),
            pltpu.SemaphoreType.DMA((2, 4)),
            pltpu.SemaphoreType.DMA((SWEEPS + 1, len(ROUTES))),
            pltpu.SemaphoreType.DMA((SWEEPS + 1, len(ROUTES))),
        ],
        compiler_params=pltpu.CompilerParams(collective_id=0, has_side_effects=True, vmem_limit_bytes=40 << 20),
    )(pltpu.with_memory_space_constraint(field, pltpu.HBM), pltpu.with_memory_space_constraint(source, pltpu.HBM))


def solution(mesh):
    spec = P("gx", "gy", "gz")
    return jax.shard_map(on_device, mesh=mesh, in_specs=(spec, spec), out_specs=spec, check_vma=False)
```

```python
import functools
import itertools

import jax
import jax.numpy as jnp
from jax import lax
from jax.experimental import pallas as pl
from jax.experimental.pallas import tpu as pltpu
from jax.sharding import PartitionSpec as P

SWEEPS = 3
HALF = 2 * SWEEPS
PAD = 16
LANES = 128
CHUNK = 8
SIXTH = 1.0 / 6.0
MESH = pl.DeviceIdType.MESH
AXES = ("gx", "gy", "gz")
ROUTES = [r for r in itertools.product((-1, 0, 1), repeat=3) if 1 <= sum(map(abs, r)) <= 2]
f32 = jnp.float32
bf16 = jnp.bfloat16


def iota(shape, dim):
    return lax.broadcasted_iota(jnp.int32, shape, dim)


def side(step):
    return 0 if step < 0 else 1


def kernel(field, source, obuf, fbuf, sbuf, S, X, own, zout, zin, xzin, yzout, yzin,
           sown, szout, szin, sxout, sxin, SC, C, U, Y, SZ, V, DZ, PK, DY, DYR, DR, DX, isem, ssem, rsem):
    M = X.shape[1] - 2
    N = X.shape[2] - 2 * PAD
    T = N // 8
    H = M // 2
    at = {a: lax.axis_index(a) for a in AXES}
    size = {a: lax.axis_size(a) for a in AXES}
    has = (at["gx"] > 0, at["gx"] < size["gx"] - 1)

    def target(route):
        return {a: lax.rem(at[a] + step + size[a], size[a]) for a, step in zip(AXES, route) if step}

    def guarded(step, action):
        if step == 0:
            action()
        else:
            pl.when(has[side(step)])(action)

    rows = pl.ds(PAD, N)
    inner = pl.ds(1, M)
    first, last = pl.ds(PAD, 8), pl.ds(PAD + N - 8, 8)
    before, after = pl.ds(PAD - 8, 8), pl.ds(PAD + N, 8)
    edge_rows = ((first, after), (last, before))

    def refs(r, route):
        x, y, z = route
        h = 2 * r
        if x:
            src_plane, dst_plane = ((1, M + 1), (M, 0))[side(x)]
        if y:
            src_rows, dst_rows = edge_rows[side(y)]
        if x and y:
            return X.at[h, src_plane, src_rows], X.at[h, dst_plane, dst_rows]
        if x and z:
            return own.at[r, src_plane - 1], xzin.at[r, side(-x), side(-z)]
        if y and z:
            return yzout.at[r, side(y)], yzin.at[r, side(-y), side(-z)]
        if x:
            return X.at[h, src_plane, rows], X.at[h, dst_plane, rows]
        if y:
            return X.at[h, inner, src_rows], X.at[h, inner, dst_rows]
        return zout.at[r, side(z)], zin.at[r, side(-z)]

    def source_refs(route):
        x, y, z = route
        if x:
            return sxout.at[side(x)], sxin.at[side(-x)]
        if y:
            src_rows, dst_rows = edge_rows[side(y)]
            return S.at[0, inner, src_rows], S.at[0, inner, dst_rows]
        return szout.at[side(z)], szin.at[side(-z)]

    def remote(r, route):
        pair = refs(r, route) if r < SWEEPS else source_refs(route)
        number = ROUTES.index(route)
        return pltpu.make_async_remote_copy(
            src_ref=pair[0], dst_ref=pair[1], send_sem=ssem.at[r, number], recv_sem=rsem.at[r, number],
            device_id=target(route), device_id_type=MESH)

    faces = [r for r in ROUTES if sum(map(abs, r)) == 1]
    edges = [r for r in ROUTES if sum(map(abs, r)) == 2]
    edges.sort(key=lambda r: abs(r[0]))
    x_faces = [r for r in faces if r[0]]
    yz_faces = [r for a in (2, 1) for r in faces if r[a]]
    yz_edges = [r for r in edges if not r[0]]
    early = [r for r in edges if r[0]] + yz_faces
    ordered = yz_edges + [q for q in faces if q[2]] + [q for q in edges if q[0]] + x_faces + [q for q in faces if q[1]]

    def start(r, routes):
        for route in routes:
            guarded(route[0], lambda route=route: remote(r, route).start())

    def wait(r, routes):
        for route in routes:
            guarded(-route[0], lambda route=route: remote(r, route).wait_recv())

    planes = 2 * M // 4
    spans = [(source, sbuf, 0, 2), (source, sbuf, 2 * M - 2, 2)]
    spans += [(field, fbuf, part * planes, planes) for part in range(4)]
    spans += [(source, sbuf, 2, 2 * M - 4)] if M > 2 else []
    loads = [
        pltpu.make_async_copy(big.at[pl.ds(first_plane, n)], small.at[pl.ds(first_plane, n)], isem.at[number])
        for number, (big, small, first_plane, n) in enumerate(spans)
    ]
    for load in loads:
        load.start()
    barrier = pltpu.get_barrier_semaphore()
    count = jnp.int32(0)
    for route in ROUTES:
        guarded(route[0], lambda route=route: pl.semaphore_signal(
            barrier, inc=1, device_id=target(route), device_id_type=MESH))
        count = count + (1 if route[0] == 0 else has[side(route[0])].astype(jnp.int32))

    lane = iota((8, LANES), 1)
    sub = iota((8, LANES), 0)
    group = lane // 4
    place = lane % 4
    odd8 = (sub + lane) % 2 == 1
    outer = (lane == 0) | (lane == LANES - 1)
    odd_rows = (iota((8 * CHUNK, LANES), 0) + iota((8 * CHUNK, LANES), 1)) % 2 == 1
    outer_rows = (iota((8 * CHUNK, LANES), 1) == 0) | (iota((8 * CHUNK, LANES), 1) == LANES - 1)
    row_of = iota((8 * CHUNK, LANES), 0)
    rim_rows = (iota((8 * CHUNK, LANES), 1) < 2) | (iota((8 * CHUNK, LANES), 1) >= LANES - 2)
    gap = jnp.abs(iota((LANES, LANES), 0) - iota((LANES, LANES), 1))
    beside_lanes = jnp.where(gap == 1, 1.0, 0.0).astype(bf16)
    beside_lanes = jnp.concatenate([beside_lanes, beside_lanes], 0)

    def turn(value, shift, axis=1):
        return pltpu.roll(value, shift % value.shape[axis], axis)

    def lane_sum(value):
        high = value.astype(bf16)
        rest = (value - high.astype(f32)).astype(bf16)
        return jnp.dot(jnp.concatenate([high, rest], 1), beside_lanes, preferred_element_type=f32)

    def swapped(value):
        where = iota(value.shape, 1) % 4
        return jnp.where(where == 1, turn(value, -1), turn(value, 1))

    zero8 = jnp.zeros((8, LANES), f32)

    def pack(acc, t, tile):
        return jnp.where(group == t, turn(tile, 4 * t + 2), acc)

    @pl.when(at["gx"] == 0)
    def _():
        for h in range(HALF):
            X[h, 0] = jnp.zeros(X.shape[2:], f32)
        for r in range(SWEEPS):
            xzin[r, 0] = jnp.zeros(xzin.shape[2:], f32)

    @pl.when(at["gx"] == size["gx"] - 1)
    def _():
        for h in range(HALF):
            X[h, M + 1] = jnp.zeros(X.shape[2:], f32)
        for r in range(SWEEPS):
            xzin[r, 1] = jnp.zeros(xzin.shape[2:], f32)

    def finish_pack(r):
        for m in range(H):
            one, two = own[r, m], own[r, m + H]
            zout[r, 0, m] = jnp.where(place >= 2, one, turn(two, -2))
            zout[r, 1, m] = jnp.where(place < 2, one, turn(two, 2))
        for m in range(M):
            yzout[r, 0, m:m + 1] = own[r, m, 0:1]
            yzout[r, 1, m:m + 1] = own[r, m, 7:8]

    V[0] = jnp.zeros((8, LANES), f32)
    V[M + 1] = jnp.zeros((8, LANES), f32)
    for k in range(2):
        DR[k, 0:8] = jnp.zeros((8, LANES), f32)
        DR[k, N + 8:N + 16] = jnp.zeros((8, LANES), f32)
    order = [0, M - 1] + list(range(1, M - 1))
    whole_odd = (iota((N, LANES), 0) + iota((N, LANES), 1)) % 2 == 1

    def split_source(m):
        even_plane, odd_plane = sbuf[2 * m], sbuf[2 * m + 1]
        value = jnp.where(whole_odd, odd_plane, even_plane)
        S[0, m + 1, rows] = value
        S[1, m + 1, rows] = jnp.where(whole_odd, even_plane, odd_plane)
        return value

    for load in loads[:2]:
        load.wait()
    for k, m in enumerate((0, M - 1)):
        value = split_source(m)
        top, bottom = value[:N // 2], pltpu.roll(value[N // 2:], 1, 1)
        sxout[k] = jnp.where(whole_odd[:N // 2], (bottom, top)[k], (top, bottom)[k])
    pl.semaphore_wait(barrier, count)
    start(SWEEPS, x_faces)

    for load in loads[2:6]:
        load.wait()
    for m in order:
        value = jnp.where(whole_odd, fbuf[2 * m], fbuf[2 * m + 1])
        X[0, m + 1, rows] = value
        acc = jnp.zeros((8, LANES), f32)
        for t in range(T):
            acc = pack(acc, t, value[8 * t:8 * t + 8])
        own[0, m] = acc
    finish_pack(0)
    start(0, ordered)

    for load in loads[6:]:
        load.wait()
    for m in range(M):
        value = S[0, m + 1, rows] if m in (0, M - 1) else split_source(m)
        acc = zero8
        for t in range(T):
            acc = pack(acc, t, value[8 * t:8 * t + 8])
        sown[m] = acc
    for q in range(-(-M // 4)):
        ends = [zero8, zero8]
        for i in range(min(4, M - 4 * q)):
            for k in range(2):
                ends[k] = jnp.where(place == i, turn(sown[4 * q + i], i - (2, 1)[k]), ends[k])
        szout[0, q], szout[1, q] = ends
    start(SWEEPS, yz_faces)

    def update(h, m, start_row, length, wings, near=None):
        here = pl.ds(start_row, length)
        centre = X[h, m + 1, here]
        if near is None:
            near = jnp.where(odd_rows[:length], X[h, m + 2, here], X[h, m, here])
        else:
            near = X[h, near + 1, here]
        total = (S[0, m + 1, here] + centre) + (near + lane_sum(centre))
        total = total + (X[h, m + 1, pl.ds(start_row - 1, length)] + X[h, m + 1, pl.ds(start_row + 1, length)])
        if wings is not None:
            total = total + jnp.where(outer_rows[:length], wings, 0.0)
        return total * f32(SIXTH)

    def inside(h, m, tiles):
        start_row, length = PAD + 8 * tiles[0], 8 * len(tiles)
        here = pl.ds(start_row, length)
        centre = X[h, m + 1, here]
        low = X[h, m, here] if m > 0 else 0.0
        high = X[h, m + 2, here] if m < M - 1 else 0.0
        if h % 2:
            low, high = high, low
        total = (S[h % 2, m + 1, here] + centre) + (jnp.where(odd_rows[:length], high, low) + lane_sum(centre))
        if tiles[0] == 0:
            down = jnp.where(row_of[:length] == 0, 0.0, pltpu.roll(centre, 1, 0))
        else:
            down = X[h, m + 1, pl.ds(start_row - 1, length)]
        if tiles[-1] == T - 1:
            above = jnp.where(row_of[:length] == length - 1, 0.0, pltpu.roll(centre, length - 1, 0))
        else:
            above = X[h, m + 1, pl.ds(start_row + 1, length)]
        return (total + (down + above)) * f32(SIXTH)

    def wings_of(edge, tiles):
        return jnp.concatenate([turn(edge, LANES - 2 - 4 * t) for t in tiles], 0)

    def spread(edge, tiles):
        return jnp.where(rim_rows[:8 * len(tiles)], wings_of(edge, tiles), 0.0)

    def shifted(value):
        above = turn(value, -1, 0)
        above = jnp.where(sub == 7, turn(above, -4), above)
        above = jnp.where((sub == 7) & (group == T - 1), 0.0, above)
        below = turn(value, 1, 0)
        below = jnp.where(sub == 0, turn(below, 4), below)
        below = jnp.where((sub == 0) & (group == 0), 0.0, below)
        return above + below

    chunks = [range(c, min(c + CHUNK, T)) for c in range(0, T, CHUNK)]
    middle = (place == 1) | (place == 2)

    def padded(tiles, low, high):
        parts = [zero8] * len(tiles)
        if tiles[0] == 0:
            parts[0] = low
        if tiles[-1] == T - 1:
            parts[-1] = high
        return jnp.concatenate(parts, 0) if tiles[0] == 0 or tiles[-1] == T - 1 else None

    for r in range(SWEEPS):
        h = 2 * r
        ended = r == SWEEPS - 1
        if r > 0:
            for m in range(1, M - 1):
                for tiles in chunks:
                    tiles = [t for t in tiles if 0 < t < T - 1]
                    here = pl.ds(PAD + 8 * tiles[0], 8 * len(tiles))
                    X[h, m + 1, here] = X[h, m + 1, here] + spread(DZ[m], tiles)
        for m in range(M):
            for tiles in chunks:
                X[h + 1, m + 1, pl.ds(PAD + 8 * tiles[0], 8 * len(tiles))] = inside(h, m, tiles)
        for m in range(M):
            acc = zero8
            for tiles in chunks:
                value = inside(h + 1, m, tiles)
                X[h + 2, m + 1, pl.ds(PAD + 8 * tiles[0], 8 * len(tiles))] = value
                if not ended and 0 < m < M - 1:
                    for t in tiles:
                        acc = pack(acc, t, value[8 * (t - tiles[0]):8 * (t - tiles[0]) + 8])
            PK[m] = acc

        wait(r, early)
        if r == 0:
            wait(SWEEPS, yz_faces)
            for m in range(M):
                q, i = divmod(m, 4)
                SC[m] = jnp.where(place == 1, turn(szin[0, q], 1 - i), turn(szin[1, q], 2 - i))
        for m in range(M):
            a, b = zin[r, 0, m % H], zin[r, 1, m % H]
            if m >= H:
                a, b = turn(a, -2), turn(b, 2)
            mine = own[r, m]
            C[m + 1] = jnp.where(place == 1, a, b)
            SZ[m] = turn(jnp.where(place == 0, a, mine), 1) + turn(jnp.where(place == 3, b, mine), -1)
        C[0] = jnp.where(place == 1, xzin[r, 0, 0], xzin[r, 0, 1])
        C[M + 1] = jnp.where(place == 1, xzin[r, 1, 0], xzin[r, 1, 1])
        U[0] = swapped(C[0])
        U[1] = swapped(C[M + 1])
        for m in range(M):
            V[m + 1] = jnp.where(middle, swapped(C[m + 1]), 0.0) * f32(SIXTH)
        for m in range(M):
            centre = C[m + 1]
            near = jnp.where(odd8, C[m + 2], C[m])
            red = (SC[m] + centre + near + (SZ[m] + shifted(centre))) * f32(SIXTH)
            mine = V[m + 1]
            near = jnp.where(odd8, V[m], V[m + 2])
            total = (swapped(red) + mine) + (near + shifted(mine))
            DZ[m] = jnp.where(middle, total, jnp.where(place == 0, turn(mine, -1), turn(mine, 1))) * f32(SIXTH)
        for k, (begin, row, end, following) in enumerate(((PAD - 8, PAD - 1, 0, 1), (PAD + N, PAD + N, 7, 6))):
            for m in range(M):
                X[h + 1, m + 1, pl.ds(begin, 8)] = update(h, m, begin, 8, None)
            change = [jnp.broadcast_to(X[h, m + 1, row:row + 1], (8, LANES)) * f32(SIXTH) for m in range(M)]
            sums = lane_sum(jnp.concatenate(change, 0))
            for m in range(M):
                low = change[m - 1] if m > 0 else 0.0
                high = change[m + 1] if m < M - 1 else 0.0
                near = jnp.where(lane % 2 == 1 - k, low, high)
                total = (X[h + 1, m + 1, row:row + 1] + change[m]) + (near + sums[8 * m:8 * m + 8])
                DY[k, m] = jnp.where(sub == end, total, jnp.where(sub == following, change[m], 0.0)) * f32(SIXTH)
                if ended:
                    DYR[k, m] = jnp.where(sub == end, change[m], 0.0)
        def black(m, tiles):
            value = X[h + 2, m + 1, pl.ds(PAD + 8 * tiles[0], 8 * len(tiles))] + spread(DZ[m], tiles)
            extra = padded(tiles, DY[0, m], DY[1, m])
            if extra is not None:
                value = value + extra
            if m in (0, M - 1):
                value = value + DX[0 if m == 0 else 1, pl.ds(8 * tiles[0], 8 * len(tiles))]
            return value

        def finished(m):
            for tiles in chunks:
                begin, length = 8 * tiles[0], 8 * len(tiles)
                value = black(m, tiles)
                red = X[h + 1, m + 1, pl.ds(PAD + begin, length)] + spread(V[m + 1], tiles)
                extra = padded(tiles, DYR[0, m], DYR[1, m])
                if extra is not None:
                    red = red + extra
                if m in (0, M - 1):
                    red = red + DR[0 if m == 0 else 1, pl.ds(8 + begin, length)]
                obuf[2 * m, pl.ds(begin, length)] = jnp.where(odd_rows[:length], value, red)
                obuf[2 * m + 1, pl.ds(begin, length)] = jnp.where(odd_rows[:length], red, value)

        if ended:
            for m in range(1, M - 1):
                finished(m)
        wait(r, x_faces)
        if r == 0:
            wait(SWEEPS, x_faces)
            for k, plane in enumerate((0, M + 1)):
                half = sxin[k]
                S[0, plane, pl.ds(PAD, N // 2)] = half
                S[0, plane, pl.ds(PAD + N // 2, N // 2)] = pltpu.roll(half, LANES - 1, 1)
        for k, (m, near) in enumerate(((-1, 0), (M, M - 1))):
            for tiles in chunks:
                begin, length = PAD + 8 * tiles[0], 8 * len(tiles)
                odd = odd_rows[:length]
                red = update(h, m, begin, length, wings_of(U[k], tiles), near)
                bare = X[h, m + 1, pl.ds(begin, length)] * f32(SIXTH)
                if k == 0:
                    red, bare = jnp.where(odd, red, 0.0), jnp.where(odd, 0.0, bare)
                else:
                    red, bare = jnp.where(odd, 0.0, red), jnp.where(odd, bare, 0.0)
                DR[k, pl.ds(8 + 8 * tiles[0], length)] = bare
                DX[k, pl.ds(8 * tiles[0], length)] = jnp.where(has[k], red, 0.0) + (bare + lane_sum(bare))
            for tiles in chunks:
                begin, length = 8 * tiles[0], 8 * len(tiles)
                here = pl.ds(begin, length)
                DX[k, here] = (DX[k, here] + (DR[k, pl.ds(7 + begin, length)] + DR[k, pl.ds(9 + begin, length)])) * f32(SIXTH)
        wait(r, yz_edges)
        small = (M, LANES)
        spot = iota(small, 1) % 4
        ends = (iota(small, 1) == 0) | (iota(small, 1) == LANES - 1)
        low_corner = jnp.where(spot == 1, yzin[r, 0, 0], yzin[r, 0, 1])
        high_corner = jnp.where(spot == 1, yzin[r, 1, 0], yzin[r, 1, 1])
        Y[0] = jnp.where(ends, turn(swapped(low_corner), LANES - 2 - 4 * (T - 1)), 0.0) * f32(1.0 / 18.0)
        Y[1] = jnp.where(ends, turn(swapped(high_corner), LANES - 2), 0.0) * f32(1.0 / 18.0)
        for m in range(M):
            for k, (end, spot) in enumerate(((0, pl.ds(0, 8)), (7, pl.ds(N - 8, 8)))):
                corner = jnp.where(sub == end, Y[k, m:m + 1], 0.0)
                if ended and 0 < m < M - 1:
                    obuf[2 * m, spot] = obuf[2 * m, spot] + jnp.where(odd8, corner, 0.0)
                    obuf[2 * m + 1, spot] = obuf[2 * m + 1, spot] + jnp.where(odd8, 0.0, corner)
                else:
                    DY[k, m] = DY[k, m] + corner

        if not ended:
            for m in (0, M - 1):
                acc = zero8
                for tiles in chunks:
                    value = black(m, tiles)
                    X[h + 2, m + 1, pl.ds(PAD + 8 * tiles[0], 8 * len(tiles))] = value
                    for t in tiles:
                        acc = pack(acc, t, value[8 * (t - tiles[0]):8 * (t - tiles[0]) + 8])
                own[r + 1, m] = acc
            for m in range(1, M - 1):
                for t in (0, T - 1):
                    X[h + 2, m + 1, pl.ds(PAD + 8 * t, 8)] = black(m, [t])
                low = jnp.where(group == 0, turn(DY[0, m], 2), 0.0)
                high = jnp.where(group == T - 1, turn(DY[1, m], 4 * T - 2), 0.0)
                own[r + 1, m] = (PK[m] + DZ[m]) + (low + high)
            finish_pack(r + 1)
            start(r + 1, ordered)
        else:
            finished(0)
            finished(M - 1)

    for r in range(SWEEPS):
        for route in ROUTES:
            guarded(route[0], lambda route=route: remote(r, route).wait_send())
    for route in faces:
        guarded(route[0], lambda route=route: remote(SWEEPS, route).wait_send())


def on_device(field, source):
    L, N, K = field.shape
    M = L // 2
    vmem = lambda *shape: pltpu.VMEM(shape, f32)
    return pl.pallas_call(
        kernel,
        out_shape=jax.ShapeDtypeStruct(field.shape, f32),
        in_specs=[pl.BlockSpec(memory_space=pltpu.HBM)] * 2,
        out_specs=pl.BlockSpec(memory_space=pltpu.VMEM),
        scratch_shapes=[
            vmem(L, N, K), vmem(L, N, K),
            vmem(2, M + 2, N + 2 * PAD, K),
            vmem(HALF + 1, M + 2, N + 2 * PAD, K),
            vmem(SWEEPS, M, 8, K),
            vmem(SWEEPS, 2, M // 2, 8, K),
            vmem(SWEEPS, 2, M // 2, 8, K),
            vmem(SWEEPS, 2, 2, 8, K),
            vmem(SWEEPS, 2, M, K),
            vmem(SWEEPS, 2, 2, M, K),
            vmem(M, 8, K),
            vmem(2, -(-M // 4), 8, K),
            vmem(2, -(-M // 4), 8, K),
            vmem(2, N // 2, K), vmem(2, N // 2, K),
            vmem(M, 8, K),
            vmem(M + 2, 8, K),
            vmem(2, 8, K),
            vmem(2, M, K),
            vmem(M, 8, K),
            vmem(M + 2, 8, K),
            vmem(M, 8, K),
            vmem(M, 8, K),
            vmem(2, M, 8, K),
            vmem(2, M, 8, K),
            vmem(2, N + 16, K),
            vmem(2, N, K),
            pltpu.SemaphoreType.DMA((7,)),
            pltpu.SemaphoreType.DMA((SWEEPS + 1, len(ROUTES))),
            pltpu.SemaphoreType.DMA((SWEEPS + 1, len(ROUTES))),
        ],
        compiler_params=pltpu.CompilerParams(collective_id=0, has_side_effects=True, vmem_limit_bytes=40 << 20),
    )(pltpu.with_memory_space_constraint(field, pltpu.HBM), pltpu.with_memory_space_constraint(source, pltpu.HBM))


def solution(mesh):
    spec = P("gx", "gy", "gz")
    return jax.shard_map(on_device, mesh=mesh, in_specs=(spec, spec), out_specs=spec, check_vma=False)
```

```python
import functools
import itertools

import jax
import jax.numpy as jnp
from jax import lax
from jax.experimental import pallas as pl
from jax.experimental.pallas import tpu as pltpu
from jax.sharding import PartitionSpec as P

SWEEPS = 3
HALF = 2 * SWEEPS
PAD = 16
LANES = 128
CHUNK = 8
SIXTH = 1.0 / 6.0
MESH = pl.DeviceIdType.MESH
AXES = ("gx", "gy", "gz")
ROUTES = [r for r in itertools.product((-1, 0, 1), repeat=3) if 1 <= sum(map(abs, r)) <= 2]
f32 = jnp.float32
bf16 = jnp.bfloat16


def iota(shape, dim):
    return lax.broadcasted_iota(jnp.int32, shape, dim)


def side(step):
    return 0 if step < 0 else 1


def kernel(field, source, obuf, fbuf, sbuf, S, X, own, zout, zin, xzin, yzout, yzin,
           sown, szout, szin, sxout, sxin, SC, C, U, Y, SZ, V, DZ, PK, DY, DYR, DR, DX, isem, ssem, rsem):
    M = X.shape[1] - 2
    N = X.shape[2] - 2 * PAD
    T = N // 8
    H = M // 2
    at = {a: lax.axis_index(a) for a in AXES}
    size = {a: lax.axis_size(a) for a in AXES}
    has = (at["gx"] > 0, at["gx"] < size["gx"] - 1)

    def target(route):
        return {a: lax.rem(at[a] + step + size[a], size[a]) for a, step in zip(AXES, route) if step}

    def guarded(step, action):
        if step == 0:
            action()
        else:
            pl.when(has[side(step)])(action)

    rows = pl.ds(PAD, N)
    inner = pl.ds(1, M)
    first, last = pl.ds(PAD, 8), pl.ds(PAD + N - 8, 8)
    before, after = pl.ds(PAD - 8, 8), pl.ds(PAD + N, 8)
    edge_rows = ((first, after), (last, before))

    def refs(r, route):
        x, y, z = route
        h = 2 * r
        if x:
            src_plane, dst_plane = ((1, M + 1), (M, 0))[side(x)]
        if y:
            src_rows, dst_rows = edge_rows[side(y)]
        if x and y:
            return X.at[h, src_plane, src_rows], X.at[h, dst_plane, dst_rows]
        if x and z:
            return own.at[r, src_plane - 1], xzin.at[r, side(-x), side(-z)]
        if y and z:
            return yzout.at[r, side(y)], yzin.at[r, side(-y), side(-z)]
        if x:
            return X.at[h, src_plane, rows], X.at[h, dst_plane, rows]
        if y:
            return X.at[h, inner, src_rows], X.at[h, inner, dst_rows]
        return zout.at[r, side(z)], zin.at[r, side(-z)]

    def source_refs(route):
        x, y, z = route
        if x:
            return sxout.at[side(x)], sxin.at[side(-x)]
        if y:
            src_rows, dst_rows = edge_rows[side(y)]
            return S.at[0, inner, src_rows], S.at[0, inner, dst_rows]
        return szout.at[side(z)], szin.at[side(-z)]

    def remote(r, route):
        pair = refs(r, route) if r < SWEEPS else source_refs(route)
        number = ROUTES.index(route)
        return pltpu.make_async_remote_copy(
            src_ref=pair[0], dst_ref=pair[1], send_sem=ssem.at[r, number], recv_sem=rsem.at[r, number],
            device_id=target(route), device_id_type=MESH)

    faces = [r for r in ROUTES if sum(map(abs, r)) == 1]
    edges = [r for r in ROUTES if sum(map(abs, r)) == 2]
    edges.sort(key=lambda r: abs(r[0]))
    x_faces = [r for r in faces if r[0]]
    yz_faces = [r for a in (2, 1) for r in faces if r[a]]
    yz_edges = [r for r in edges if not r[0]]
    early = [r for r in edges if r[0]] + yz_faces
    ordered = yz_edges + [q for q in faces if q[2]] + [q for q in edges if q[0]] + x_faces + [q for q in faces if q[1]]

    def start(r, routes):
        for route in routes:
            guarded(route[0], lambda route=route: remote(r, route).start())

    def wait(r, routes):
        for route in routes:
            guarded(-route[0], lambda route=route: remote(r, route).wait_recv())

    barrier = pltpu.get_barrier_semaphore()
    count = jnp.int32(0)
    for route in ordered:
        guarded(route[0], lambda route=route: pl.semaphore_signal(
            barrier, inc=1, device_id=target(route), device_id_type=MESH))
        count = count + (1 if route[0] == 0 else has[side(route[0])].astype(jnp.int32))

    planes = 2 * M // 4
    spans = [(source, sbuf, 0, 2), (source, sbuf, 2 * M - 2, 2)]
    spans += [(field, fbuf, part * planes, planes) for part in range(4)]
    spans += [(source, sbuf, 2, 2 * M - 4)] if M > 2 else []
    loads = [
        pltpu.make_async_copy(big.at[pl.ds(first_plane, n)], small.at[pl.ds(first_plane, n)], isem.at[number])
        for number, (big, small, first_plane, n) in enumerate(spans)
    ]
    for load in loads:
        load.start()
    lane = iota((8, LANES), 1)
    sub = iota((8, LANES), 0)
    group = lane // 4
    place = lane % 4
    odd8 = (sub + lane) % 2 == 1
    outer = (lane == 0) | (lane == LANES - 1)
    odd_rows = (iota((8 * CHUNK, LANES), 0) + iota((8 * CHUNK, LANES), 1)) % 2 == 1
    outer_rows = (iota((8 * CHUNK, LANES), 1) == 0) | (iota((8 * CHUNK, LANES), 1) == LANES - 1)
    row_of = iota((8 * CHUNK, LANES), 0)
    rim_rows = (iota((8 * CHUNK, LANES), 1) < 2) | (iota((8 * CHUNK, LANES), 1) >= LANES - 2)
    gap = jnp.abs(iota((LANES, LANES), 0) - iota((LANES, LANES), 1))
    beside_lanes = jnp.where(gap == 1, 1.0, 0.0).astype(bf16)
    beside_lanes = jnp.concatenate([beside_lanes, beside_lanes], 0)

    def turn(value, shift, axis=1):
        return pltpu.roll(value, shift % value.shape[axis], axis)

    def lane_sum(value):
        high = value.astype(bf16)
        rest = (value - high.astype(f32)).astype(bf16)
        return jnp.dot(jnp.concatenate([high, rest], 1), beside_lanes, preferred_element_type=f32)

    def swapped(value):
        where = iota(value.shape, 1) % 4
        return jnp.where(where == 1, turn(value, -1), turn(value, 1))

    zero8 = jnp.zeros((8, LANES), f32)

    def pack(acc, t, tile):
        return jnp.where(group == t, turn(tile, 4 * t + 2), acc)

    @pl.when(at["gx"] == 0)
    def _():
        for h in range(HALF):
            X[h, 0] = jnp.zeros(X.shape[2:], f32)
        for r in range(SWEEPS):
            xzin[r, 0] = jnp.zeros(xzin.shape[2:], f32)

    @pl.when(at["gx"] == size["gx"] - 1)
    def _():
        for h in range(HALF):
            X[h, M + 1] = jnp.zeros(X.shape[2:], f32)
        for r in range(SWEEPS):
            xzin[r, 1] = jnp.zeros(xzin.shape[2:], f32)

    def finish_pack(r):
        for m in range(H):
            one, two = own[r, m], own[r, m + H]
            zout[r, 0, m] = jnp.where(place >= 2, one, turn(two, -2))
            zout[r, 1, m] = jnp.where(place < 2, one, turn(two, 2))
        for m in range(M):
            yzout[r, 0, m:m + 1] = own[r, m, 0:1]
            yzout[r, 1, m:m + 1] = own[r, m, 7:8]

    V[0] = jnp.zeros((8, LANES), f32)
    V[M + 1] = jnp.zeros((8, LANES), f32)
    for k in range(2):
        DR[k, 0:8] = jnp.zeros((8, LANES), f32)
        DR[k, N + 8:N + 16] = jnp.zeros((8, LANES), f32)
    order = [0, M - 1] + list(range(1, M - 1))
    whole_odd = (iota((N, LANES), 0) + iota((N, LANES), 1)) % 2 == 1

    def split_source(m):
        even_plane, odd_plane = sbuf[2 * m], sbuf[2 * m + 1]
        value = jnp.where(whole_odd, odd_plane, even_plane)
        S[0, m + 1, rows] = value
        S[1, m + 1, rows] = jnp.where(whole_odd, even_plane, odd_plane)
        return value

    for load in loads[:2]:
        load.wait()
    for k, m in enumerate((0, M - 1)):
        value = split_source(m)
        top, bottom = value[:N // 2], pltpu.roll(value[N // 2:], 1, 1)
        sxout[k] = jnp.where(whole_odd[:N // 2], (bottom, top)[k], (top, bottom)[k])
    pl.semaphore_wait(barrier, count)
    start(SWEEPS, x_faces)

    for load in loads[2:6]:
        load.wait()
    for m in order:
        value = jnp.where(whole_odd, fbuf[2 * m], fbuf[2 * m + 1])
        X[0, m + 1, rows] = value
        acc = jnp.zeros((8, LANES), f32)
        for t in range(T):
            acc = pack(acc, t, value[8 * t:8 * t + 8])
        own[0, m] = acc
    finish_pack(0)
    start(0, ordered)

    for load in loads[6:]:
        load.wait()
    for m in range(M):
        value = S[0, m + 1, rows] if m in (0, M - 1) else split_source(m)
        acc = zero8
        for t in range(T):
            acc = pack(acc, t, value[8 * t:8 * t + 8])
        sown[m] = acc
    for q in range(-(-M // 4)):
        ends = [zero8, zero8]
        for i in range(min(4, M - 4 * q)):
            for k in range(2):
                ends[k] = jnp.where(place == i, turn(sown[4 * q + i], i - (2, 1)[k]), ends[k])
        szout[0, q], szout[1, q] = ends
    start(SWEEPS, yz_faces)

    def update(h, m, start_row, length, wings, near=None):
        here = pl.ds(start_row, length)
        centre = X[h, m + 1, here]
        if near is None:
            near = jnp.where(odd_rows[:length], X[h, m + 2, here], X[h, m, here])
        else:
            near = X[h, near + 1, here]
        total = (S[0, m + 1, here] + centre) + (near + lane_sum(centre))
        total = total + (X[h, m + 1, pl.ds(start_row - 1, length)] + X[h, m + 1, pl.ds(start_row + 1, length)])
        if wings is not None:
            total = total + jnp.where(outer_rows[:length], wings, 0.0)
        return total * f32(SIXTH)

    def inside(h, m, tiles):
        start_row, length = PAD + 8 * tiles[0], 8 * len(tiles)
        here = pl.ds(start_row, length)
        centre = X[h, m + 1, here]
        low = X[h, m, here] if m > 0 else 0.0
        high = X[h, m + 2, here] if m < M - 1 else 0.0
        if h % 2:
            low, high = high, low
        total = (S[h % 2, m + 1, here] + centre) + (jnp.where(odd_rows[:length], high, low) + lane_sum(centre))
        if tiles[0] == 0:
            down = jnp.where(row_of[:length] == 0, 0.0, pltpu.roll(centre, 1, 0))
        else:
            down = X[h, m + 1, pl.ds(start_row - 1, length)]
        if tiles[-1] == T - 1:
            above = jnp.where(row_of[:length] == length - 1, 0.0, pltpu.roll(centre, length - 1, 0))
        else:
            above = X[h, m + 1, pl.ds(start_row + 1, length)]
        return (total + (down + above)) * f32(SIXTH)

    def wings_of(edge, tiles):
        return jnp.concatenate([turn(edge, LANES - 2 - 4 * t) for t in tiles], 0)

    def spread(edge, tiles):
        return jnp.where(rim_rows[:8 * len(tiles)], wings_of(edge, tiles), 0.0)

    def shifted(value):
        above = turn(value, -1, 0)
        above = jnp.where(sub == 7, turn(above, -4), above)
        above = jnp.where((sub == 7) & (group == T - 1), 0.0, above)
        below = turn(value, 1, 0)
        below = jnp.where(sub == 0, turn(below, 4), below)
        below = jnp.where((sub == 0) & (group == 0), 0.0, below)
        return above + below

    chunks = [range(c, min(c + CHUNK, T)) for c in range(0, T, CHUNK)]
    middle = (place == 1) | (place == 2)

    def padded(tiles, low, high):
        parts = [zero8] * len(tiles)
        if tiles[0] == 0:
            parts[0] = low
        if tiles[-1] == T - 1:
            parts[-1] = high
        return jnp.concatenate(parts, 0) if tiles[0] == 0 or tiles[-1] == T - 1 else None

    for r in range(SWEEPS):
        h = 2 * r
        ended = r == SWEEPS - 1
        if r > 0:
            for m in range(1, M - 1):
                for tiles in chunks:
                    tiles = [t for t in tiles if 0 < t < T - 1]
                    here = pl.ds(PAD + 8 * tiles[0], 8 * len(tiles))
                    X[h, m + 1, here] = X[h, m + 1, here] + spread(DZ[m], tiles)
        for m in range(M):
            for tiles in chunks:
                X[h + 1, m + 1, pl.ds(PAD + 8 * tiles[0], 8 * len(tiles))] = inside(h, m, tiles)
        for m in range(M):
            acc = zero8
            for tiles in chunks:
                value = inside(h + 1, m, tiles)
                X[h + 2, m + 1, pl.ds(PAD + 8 * tiles[0], 8 * len(tiles))] = value
                if not ended and 0 < m < M - 1:
                    for t in tiles:
                        acc = pack(acc, t, value[8 * (t - tiles[0]):8 * (t - tiles[0]) + 8])
            PK[m] = acc

        wait(r, early)
        if r == 0:
            wait(SWEEPS, yz_faces)
            for m in range(M):
                q, i = divmod(m, 4)
                SC[m] = jnp.where(place == 1, turn(szin[0, q], 1 - i), turn(szin[1, q], 2 - i))
        for m in range(M):
            a, b = zin[r, 0, m % H], zin[r, 1, m % H]
            if m >= H:
                a, b = turn(a, -2), turn(b, 2)
            mine = own[r, m]
            C[m + 1] = jnp.where(place == 1, a, b)
            SZ[m] = turn(jnp.where(place == 0, a, mine), 1) + turn(jnp.where(place == 3, b, mine), -1)
        C[0] = jnp.where(place == 1, xzin[r, 0, 0], xzin[r, 0, 1])
        C[M + 1] = jnp.where(place == 1, xzin[r, 1, 0], xzin[r, 1, 1])
        U[0] = swapped(C[0])
        U[1] = swapped(C[M + 1])
        for m in range(M):
            V[m + 1] = jnp.where(middle, swapped(C[m + 1]), 0.0) * f32(SIXTH)
        for m in range(M):
            centre = C[m + 1]
            near = jnp.where(odd8, C[m + 2], C[m])
            red = (SC[m] + centre + near + (SZ[m] + shifted(centre))) * f32(SIXTH)
            mine = V[m + 1]
            near = jnp.where(odd8, V[m], V[m + 2])
            total = (swapped(red) + mine) + (near + shifted(mine))
            DZ[m] = jnp.where(middle, total, jnp.where(place == 0, turn(mine, -1), turn(mine, 1))) * f32(SIXTH)
        for k, (begin, row, end, following) in enumerate(((PAD - 8, PAD - 1, 0, 1), (PAD + N, PAD + N, 7, 6))):
            for m in range(M):
                X[h + 1, m + 1, pl.ds(begin, 8)] = update(h, m, begin, 8, None)
            change = [jnp.broadcast_to(X[h, m + 1, row:row + 1], (8, LANES)) * f32(SIXTH) for m in range(M)]
            sums = lane_sum(jnp.concatenate(change, 0))
            for m in range(M):
                low = change[m - 1] if m > 0 else 0.0
                high = change[m + 1] if m < M - 1 else 0.0
                near = jnp.where(lane % 2 == 1 - k, low, high)
                total = (X[h + 1, m + 1, row:row + 1] + change[m]) + (near + sums[8 * m:8 * m + 8])
                DY[k, m] = jnp.where(sub == end, total, jnp.where(sub == following, change[m], 0.0)) * f32(SIXTH)
                if ended:
                    DYR[k, m] = jnp.where(sub == end, change[m], 0.0)
        def black(m, tiles):
            value = X[h + 2, m + 1, pl.ds(PAD + 8 * tiles[0], 8 * len(tiles))] + spread(DZ[m], tiles)
            extra = padded(tiles, DY[0, m], DY[1, m])
            if extra is not None:
                value = value + extra
            if m in (0, M - 1):
                value = value + DX[0 if m == 0 else 1, pl.ds(8 * tiles[0], 8 * len(tiles))]
            return value

        def finished(m):
            for tiles in chunks:
                begin, length = 8 * tiles[0], 8 * len(tiles)
                value = black(m, tiles)
                red = X[h + 1, m + 1, pl.ds(PAD + begin, length)] + spread(V[m + 1], tiles)
                extra = padded(tiles, DYR[0, m], DYR[1, m])
                if extra is not None:
                    red = red + extra
                if m in (0, M - 1):
                    red = red + DR[0 if m == 0 else 1, pl.ds(8 + begin, length)]
                obuf[2 * m, pl.ds(begin, length)] = jnp.where(odd_rows[:length], value, red)
                obuf[2 * m + 1, pl.ds(begin, length)] = jnp.where(odd_rows[:length], red, value)

        if ended:
            for m in range(1, M - 1):
                finished(m)
        wait(r, x_faces)
        if r == 0:
            wait(SWEEPS, x_faces)
            for k, plane in enumerate((0, M + 1)):
                half = sxin[k]
                S[0, plane, pl.ds(PAD, N // 2)] = half
                S[0, plane, pl.ds(PAD + N // 2, N // 2)] = pltpu.roll(half, LANES - 1, 1)
        for k, (plane, near) in enumerate(((0, 1), (M + 1, M))):
            for tiles in chunks:
                length = 8 * len(tiles)
                bare = X[h, plane, pl.ds(PAD + 8 * tiles[0], length)] * f32(SIXTH)
                odd = odd_rows[:length]
                DR[k, pl.ds(8 + 8 * tiles[0], length)] = jnp.where(odd, bare, 0.0) if k else jnp.where(odd, 0.0, bare)
            for tiles in chunks:
                begin, length = 8 * tiles[0], 8 * len(tiles)
                here, odd = pl.ds(PAD + begin, length), odd_rows[:length]
                bare = DR[k, pl.ds(8 + begin, length)]
                around = lane_sum(bare) + (DR[k, pl.ds(7 + begin, length)] + DR[k, pl.ds(9 + begin, length)])
                rest = (S[0, plane, here] + X[h, plane, here]) + X[h, near, here]
                rest = rest + jnp.where(outer_rows[:length], wings_of(U[k], tiles), 0.0)
                if tiles[0] == 0:
                    rest = rest + jnp.where(row_of[:length] == 0, X[h, plane, PAD - 1:PAD], 0.0)
                if tiles[-1] == T - 1:
                    rest = rest + jnp.where(row_of[:length] == length - 1, X[h, plane, PAD + N:PAD + N + 1], 0.0)
                red = rest * f32(SIXTH) + around
                red = jnp.where(odd, 0.0, red) if k else jnp.where(odd, red, 0.0)
                DX[k, pl.ds(begin, length)] = (jnp.where(has[k], red, 0.0) + (bare + around)) * f32(SIXTH)
        wait(r, yz_edges)
        small = (M, LANES)
        spot = iota(small, 1) % 4
        ends = (iota(small, 1) == 0) | (iota(small, 1) == LANES - 1)
        low_corner = jnp.where(spot == 1, yzin[r, 0, 0], yzin[r, 0, 1])
        high_corner = jnp.where(spot == 1, yzin[r, 1, 0], yzin[r, 1, 1])
        Y[0] = jnp.where(ends, turn(swapped(low_corner), LANES - 2 - 4 * (T - 1)), 0.0) * f32(1.0 / 18.0)
        Y[1] = jnp.where(ends, turn(swapped(high_corner), LANES - 2), 0.0) * f32(1.0 / 18.0)
        for m in range(M):
            for k, (end, spot) in enumerate(((0, pl.ds(0, 8)), (7, pl.ds(N - 8, 8)))):
                corner = jnp.where(sub == end, Y[k, m:m + 1], 0.0)
                if ended and 0 < m < M - 1:
                    obuf[2 * m, spot] = obuf[2 * m, spot] + jnp.where(odd8, corner, 0.0)
                    obuf[2 * m + 1, spot] = obuf[2 * m + 1, spot] + jnp.where(odd8, 0.0, corner)
                else:
                    DY[k, m] = DY[k, m] + corner

        if not ended:
            for m in (0, M - 1):
                acc = zero8
                for tiles in chunks:
                    value = black(m, tiles)
                    X[h + 2, m + 1, pl.ds(PAD + 8 * tiles[0], 8 * len(tiles))] = value
                    for t in tiles:
                        acc = pack(acc, t, value[8 * (t - tiles[0]):8 * (t - tiles[0]) + 8])
                own[r + 1, m] = acc
            for m in range(1, M - 1):
                for t in (0, T - 1):
                    X[h + 2, m + 1, pl.ds(PAD + 8 * t, 8)] = black(m, [t])
                low = jnp.where(group == 0, turn(DY[0, m], 2), 0.0)
                high = jnp.where(group == T - 1, turn(DY[1, m], 4 * T - 2), 0.0)
                own[r + 1, m] = (PK[m] + DZ[m]) + (low + high)
            finish_pack(r + 1)
            start(r + 1, ordered)
        else:
            finished(0)
            finished(M - 1)

    for r in range(SWEEPS):
        for route in ROUTES:
            guarded(route[0], lambda route=route: remote(r, route).wait_send())
    for route in faces:
        guarded(route[0], lambda route=route: remote(SWEEPS, route).wait_send())


def on_device(field, source):
    L, N, K = field.shape
    M = L // 2
    vmem = lambda *shape: pltpu.VMEM(shape, f32)
    return pl.pallas_call(
        kernel,
        out_shape=jax.ShapeDtypeStruct(field.shape, f32),
        in_specs=[pl.BlockSpec(memory_space=pltpu.HBM)] * 2,
        out_specs=pl.BlockSpec(memory_space=pltpu.VMEM),
        scratch_shapes=[
            vmem(L, N, K), vmem(L, N, K),
            vmem(2, M + 2, N + 2 * PAD, K),
            vmem(HALF + 1, M + 2, N + 2 * PAD, K),
            vmem(SWEEPS, M, 8, K),
            vmem(SWEEPS, 2, M // 2, 8, K),
            vmem(SWEEPS, 2, M // 2, 8, K),
            vmem(SWEEPS, 2, 2, 8, K),
            vmem(SWEEPS, 2, M, K),
            vmem(SWEEPS, 2, 2, M, K),
            vmem(M, 8, K),
            vmem(2, -(-M // 4), 8, K),
            vmem(2, -(-M // 4), 8, K),
            vmem(2, N // 2, K), vmem(2, N // 2, K),
            vmem(M, 8, K),
            vmem(M + 2, 8, K),
            vmem(2, 8, K),
            vmem(2, M, K),
            vmem(M, 8, K),
            vmem(M + 2, 8, K),
            vmem(M, 8, K),
            vmem(M, 8, K),
            vmem(2, M, 8, K),
            vmem(2, M, 8, K),
            vmem(2, N + 16, K),
            vmem(2, N, K),
            pltpu.SemaphoreType.DMA((7,)),
            pltpu.SemaphoreType.DMA((SWEEPS + 1, len(ROUTES))),
            pltpu.SemaphoreType.DMA((SWEEPS + 1, len(ROUTES))),
        ],
        compiler_params=pltpu.CompilerParams(collective_id=0, has_side_effects=True, vmem_limit_bytes=40 << 20),
    )(pltpu.with_memory_space_constraint(field, pltpu.HBM), pltpu.with_memory_space_constraint(source, pltpu.HBM))


def solution(mesh):
    spec = P("gx", "gy", "gz")
    return jax.shard_map(on_device, mesh=mesh, in_specs=(spec, spec), out_specs=spec, check_vma=False)
```

```python
import functools
import itertools

import jax
import jax.numpy as jnp
from jax import lax
from jax.experimental import pallas as pl
from jax.experimental.pallas import tpu as pltpu
from jax.sharding import PartitionSpec as P

SWEEPS = 3
HALF = 2 * SWEEPS
PAD = 16
LANES = 128
CHUNK = 16
SIXTH = 1.0 / 6.0
MESH = pl.DeviceIdType.MESH
AXES = ("gx", "gy", "gz")
ROUTES = [r for r in itertools.product((-1, 0, 1), repeat=3) if 1 <= sum(map(abs, r)) <= 2]
f32 = jnp.float32
bf16 = jnp.bfloat16


def iota(shape, dim):
    return lax.broadcasted_iota(jnp.int32, shape, dim)


def side(step):
    return 0 if step < 0 else 1


def kernel(field, source, obuf, fbuf, sbuf, S, X, own, zout, zin, xzin, yzout, yzin,
           sown, szout, szin, sxout, sxin, SC, C, U, Y, SZ, V, DZ, PK, DY, DYR, DR, DX, isem, ssem, rsem):
    M = X.shape[1] - 2
    N = X.shape[2] - 2 * PAD
    T = N // 8
    H = M // 2
    at = {a: lax.axis_index(a) for a in AXES}
    size = {a: lax.axis_size(a) for a in AXES}
    has = (at["gx"] > 0, at["gx"] < size["gx"] - 1)

    def target(route):
        return {a: lax.rem(at[a] + step + size[a], size[a]) for a, step in zip(AXES, route) if step}

    def guarded(step, action):
        if step == 0:
            action()
        else:
            pl.when(has[side(step)])(action)

    rows = pl.ds(PAD, N)
    inner = pl.ds(1, M)
    first, last = pl.ds(PAD, 8), pl.ds(PAD + N - 8, 8)
    before, after = pl.ds(PAD - 8, 8), pl.ds(PAD + N, 8)
    edge_rows = ((first, after), (last, before))

    def refs(r, route):
        x, y, z = route
        h = 2 * r
        if x:
            src_plane, dst_plane = ((1, M + 1), (M, 0))[side(x)]
        if y:
            src_rows, dst_rows = edge_rows[side(y)]
        if x and y:
            return X.at[h, src_plane, src_rows], X.at[h, dst_plane, dst_rows]
        if x and z:
            return own.at[r, src_plane - 1], xzin.at[r, side(-x), side(-z)]
        if y and z:
            return yzout.at[r, side(y)], yzin.at[r, side(-y), side(-z)]
        if x:
            return X.at[h, src_plane, rows], X.at[h, dst_plane, rows]
        if y:
            return X.at[h, inner, src_rows], X.at[h, inner, dst_rows]
        return zout.at[r, side(z)], zin.at[r, side(-z)]

    def source_refs(route):
        x, y, z = route
        if x:
            return sxout.at[side(x)], sxin.at[side(-x)]
        if y:
            src_rows, dst_rows = edge_rows[side(y)]
            return S.at[0, inner, src_rows], S.at[0, inner, dst_rows]
        return szout.at[side(z)], szin.at[side(-z)]

    def remote(r, route):
        pair = refs(r, route) if r < SWEEPS else source_refs(route)
        number = ROUTES.index(route)
        return pltpu.make_async_remote_copy(
            src_ref=pair[0], dst_ref=pair[1], send_sem=ssem.at[r, number], recv_sem=rsem.at[r, number],
            device_id=target(route), device_id_type=MESH)

    faces = [r for r in ROUTES if sum(map(abs, r)) == 1]
    edges = [r for r in ROUTES if sum(map(abs, r)) == 2]
    edges.sort(key=lambda r: abs(r[0]))
    x_faces = [r for r in faces if r[0]]
    yz_faces = [r for a in (2, 1) for r in faces if r[a]]
    yz_edges = [r for r in edges if not r[0]]
    early = [r for r in edges if r[0]] + yz_faces
    ordered = yz_edges + [q for q in faces if q[2]] + [q for q in edges if q[0]] + x_faces + [q for q in faces if q[1]]

    def start(r, routes):
        for route in routes:
            guarded(route[0], lambda route=route: remote(r, route).start())

    def wait(r, routes):
        for route in routes:
            guarded(-route[0], lambda route=route: remote(r, route).wait_recv())

    barrier = pltpu.get_barrier_semaphore()
    count = jnp.int32(0)
    for route in ordered:
        guarded(route[0], lambda route=route: pl.semaphore_signal(
            barrier, inc=1, device_id=target(route), device_id_type=MESH))
        count = count + (1 if route[0] == 0 else has[side(route[0])].astype(jnp.int32))

    planes = 2 * M // 4
    spans = [(source, sbuf, 0, 2), (source, sbuf, 2 * M - 2, 2)]
    spans += [(field, fbuf, part * planes, planes) for part in range(4)]
    spans += [(source, sbuf, 2, 2 * M - 4)] if M > 2 else []
    loads = [
        pltpu.make_async_copy(big.at[pl.ds(first_plane, n)], small.at[pl.ds(first_plane, n)], isem.at[number])
        for number, (big, small, first_plane, n) in enumerate(spans)
    ]
    for load in loads:
        load.start()
    lane = iota((8, LANES), 1)
    sub = iota((8, LANES), 0)
    group = lane // 4
    place = lane % 4
    odd8 = (sub + lane) % 2 == 1
    outer = (lane == 0) | (lane == LANES - 1)
    odd_rows = (iota((8 * CHUNK, LANES), 0) + iota((8 * CHUNK, LANES), 1)) % 2 == 1
    outer_rows = (iota((8 * CHUNK, LANES), 1) == 0) | (iota((8 * CHUNK, LANES), 1) == LANES - 1)
    row_of = iota((8 * CHUNK, LANES), 0)
    rim_rows = (iota((8 * CHUNK, LANES), 1) < 2) | (iota((8 * CHUNK, LANES), 1) >= LANES - 2)
    gap = jnp.abs(iota((LANES, LANES), 0) - iota((LANES, LANES), 1))
    beside_lanes = jnp.where(gap == 1, 1.0, 0.0).astype(bf16)
    beside_lanes = jnp.concatenate([beside_lanes, beside_lanes], 0)

    def turn(value, shift, axis=1):
        return pltpu.roll(value, shift % value.shape[axis], axis)

    def lane_sum(value):
        high = value.astype(bf16)
        rest = (value - high.astype(f32)).astype(bf16)
        return jnp.dot(jnp.concatenate([high, rest], 1), beside_lanes, preferred_element_type=f32)

    def swapped(value):
        where = iota(value.shape, 1) % 4
        return jnp.where(where == 1, turn(value, -1), turn(value, 1))

    zero8 = jnp.zeros((8, LANES), f32)

    def pack(acc, t, tile):
        return jnp.where(group == t, turn(tile, 4 * t + 2), acc)

    @pl.when(at["gx"] == 0)
    def _():
        for h in range(HALF):
            X[h, 0] = jnp.zeros(X.shape[2:], f32)
        for r in range(SWEEPS):
            xzin[r, 0] = jnp.zeros(xzin.shape[2:], f32)

    @pl.when(at["gx"] == size["gx"] - 1)
    def _():
        for h in range(HALF):
            X[h, M + 1] = jnp.zeros(X.shape[2:], f32)
        for r in range(SWEEPS):
            xzin[r, 1] = jnp.zeros(xzin.shape[2:], f32)

    def finish_pack(r):
        for m in range(H):
            one, two = own[r, m], own[r, m + H]
            zout[r, 0, m] = jnp.where(place >= 2, one, turn(two, -2))
            zout[r, 1, m] = jnp.where(place < 2, one, turn(two, 2))
        for m in range(M):
            yzout[r, 0, m:m + 1] = own[r, m, 0:1]
            yzout[r, 1, m:m + 1] = own[r, m, 7:8]

    V[0] = jnp.zeros((8, LANES), f32)
    V[M + 1] = jnp.zeros((8, LANES), f32)
    for k in range(2):
        DR[k, 0:8] = jnp.zeros((8, LANES), f32)
        DR[k, N + 8:N + 16] = jnp.zeros((8, LANES), f32)
    order = [0, M - 1] + list(range(1, M - 1))
    whole_odd = (iota((N, LANES), 0) + iota((N, LANES), 1)) % 2 == 1

    def split_source(m):
        even_plane, odd_plane = sbuf[2 * m], sbuf[2 * m + 1]
        value = jnp.where(whole_odd, odd_plane, even_plane)
        S[0, m + 1, rows] = value
        S[1, m + 1, rows] = jnp.where(whole_odd, even_plane, odd_plane)
        return value

    for load in loads[:2]:
        load.wait()
    for k, m in enumerate((0, M - 1)):
        value = split_source(m)
        top, bottom = value[:N // 2], pltpu.roll(value[N // 2:], 1, 1)
        sxout[k] = jnp.where(whole_odd[:N // 2], (bottom, top)[k], (top, bottom)[k])

    for load in loads[2:6]:
        load.wait()
    for m in order:
        value = jnp.where(whole_odd, fbuf[2 * m], fbuf[2 * m + 1])
        X[0, m + 1, rows] = value
        acc = jnp.zeros((8, LANES), f32)
        for t in range(T):
            acc = pack(acc, t, value[8 * t:8 * t + 8])
        own[0, m] = acc
    finish_pack(0)
    pl.semaphore_wait(barrier, count)
    start(0, ordered)
    start(SWEEPS, x_faces)

    for load in loads[6:]:
        load.wait()
    for m in range(M):
        value = S[0, m + 1, rows] if m in (0, M - 1) else split_source(m)
        acc = zero8
        for t in range(T):
            acc = pack(acc, t, value[8 * t:8 * t + 8])
        sown[m] = acc
    for q in range(-(-M // 4)):
        ends = [zero8, zero8]
        for i in range(min(4, M - 4 * q)):
            for k in range(2):
                ends[k] = jnp.where(place == i, turn(sown[4 * q + i], i - (2, 1)[k]), ends[k])
        szout[0, q], szout[1, q] = ends
    start(SWEEPS, yz_faces)

    def update(h, m, start_row, length, wings, near=None):
        here = pl.ds(start_row, length)
        centre = X[h, m + 1, here]
        if near is None:
            near = jnp.where(odd_rows[:length], X[h, m + 2, here], X[h, m, here])
        else:
            near = X[h, near + 1, here]
        total = (S[0, m + 1, here] + centre) + (near + lane_sum(centre))
        total = total + (X[h, m + 1, pl.ds(start_row - 1, length)] + X[h, m + 1, pl.ds(start_row + 1, length)])
        if wings is not None:
            total = total + jnp.where(outer_rows[:length], wings, 0.0)
        return total * f32(SIXTH)

    def inside(h, m, tiles):
        start_row, length = PAD + 8 * tiles[0], 8 * len(tiles)
        here = pl.ds(start_row, length)
        centre = X[h, m + 1, here]
        low = X[h, m, here] if m > 0 else 0.0
        high = X[h, m + 2, here] if m < M - 1 else 0.0
        if h % 2:
            low, high = high, low
        total = (S[h % 2, m + 1, here] + centre) + (jnp.where(odd_rows[:length], high, low) + lane_sum(centre))
        if tiles[0] == 0:
            down = jnp.where(row_of[:length] == 0, 0.0, pltpu.roll(centre, 1, 0))
        else:
            down = X[h, m + 1, pl.ds(start_row - 1, length)]
        if tiles[-1] == T - 1:
            above = jnp.where(row_of[:length] == length - 1, 0.0, pltpu.roll(centre, length - 1, 0))
        else:
            above = X[h, m + 1, pl.ds(start_row + 1, length)]
        return (total + (down + above)) * f32(SIXTH)

    def wings_of(edge, tiles):
        return jnp.concatenate([turn(edge, LANES - 2 - 4 * t) for t in tiles], 0)

    def spread(edge, tiles):
        return jnp.where(rim_rows[:8 * len(tiles)], wings_of(edge, tiles), 0.0)

    def shifted(value):
        above = turn(value, -1, 0)
        above = jnp.where(sub == 7, turn(above, -4), above)
        above = jnp.where((sub == 7) & (group == T - 1), 0.0, above)
        below = turn(value, 1, 0)
        below = jnp.where(sub == 0, turn(below, 4), below)
        below = jnp.where((sub == 0) & (group == 0), 0.0, below)
        return above + below

    chunks = [range(c, min(c + CHUNK, T)) for c in range(0, T, CHUNK)]
    middle = (place == 1) | (place == 2)

    def padded(tiles, low, high):
        parts = [zero8] * len(tiles)
        if tiles[0] == 0:
            parts[0] = low
        if tiles[-1] == T - 1:
            parts[-1] = high
        return jnp.concatenate(parts, 0) if tiles[0] == 0 or tiles[-1] == T - 1 else None

    for r in range(SWEEPS):
        h = 2 * r
        ended = r == SWEEPS - 1
        if r > 0:
            for m in range(1, M - 1):
                for tiles in chunks:
                    tiles = [t for t in tiles if 0 < t < T - 1]
                    here = pl.ds(PAD + 8 * tiles[0], 8 * len(tiles))
                    X[h, m + 1, here] = X[h, m + 1, here] + spread(DZ[m], tiles)
        for m in range(M):
            for tiles in chunks:
                X[h + 1, m + 1, pl.ds(PAD + 8 * tiles[0], 8 * len(tiles))] = inside(h, m, tiles)
        for m in range(M):
            acc = zero8
            for tiles in chunks:
                value = inside(h + 1, m, tiles)
                X[h + 2, m + 1, pl.ds(PAD + 8 * tiles[0], 8 * len(tiles))] = value
                if not ended and 0 < m < M - 1:
                    for t in tiles:
                        acc = pack(acc, t, value[8 * (t - tiles[0]):8 * (t - tiles[0]) + 8])
            PK[m] = acc

        wait(r, early)
        if r == 0:
            wait(SWEEPS, yz_faces)
            for m in range(M):
                q, i = divmod(m, 4)
                SC[m] = jnp.where(place == 1, turn(szin[0, q], 1 - i), turn(szin[1, q], 2 - i))
        for m in range(M):
            a, b = zin[r, 0, m % H], zin[r, 1, m % H]
            if m >= H:
                a, b = turn(a, -2), turn(b, 2)
            mine = own[r, m]
            C[m + 1] = jnp.where(place == 1, a, b)
            SZ[m] = turn(jnp.where(place == 0, a, mine), 1) + turn(jnp.where(place == 3, b, mine), -1)
        C[0] = jnp.where(place == 1, xzin[r, 0, 0], xzin[r, 0, 1])
        C[M + 1] = jnp.where(place == 1, xzin[r, 1, 0], xzin[r, 1, 1])
        U[0] = swapped(C[0])
        U[1] = swapped(C[M + 1])
        for m in range(M):
            V[m + 1] = jnp.where(middle, swapped(C[m + 1]), 0.0) * f32(SIXTH)
        for m in range(M):
            centre = C[m + 1]
            near = jnp.where(odd8, C[m + 2], C[m])
            red = (SC[m] + centre + near + (SZ[m] + shifted(centre))) * f32(SIXTH)
            mine = V[m + 1]
            near = jnp.where(odd8, V[m], V[m + 2])
            total = (swapped(red) + mine) + (near + shifted(mine))
            DZ[m] = jnp.where(middle, total, jnp.where(place == 0, turn(mine, -1), turn(mine, 1))) * f32(SIXTH)
        for k, (begin, row, end, following) in enumerate(((PAD - 8, PAD - 1, 0, 1), (PAD + N, PAD + N, 7, 6))):
            for m in range(M):
                X[h + 1, m + 1, pl.ds(begin, 8)] = update(h, m, begin, 8, None)
            change = [jnp.broadcast_to(X[h, m + 1, row:row + 1], (8, LANES)) * f32(SIXTH) for m in range(M)]
            sums = lane_sum(jnp.concatenate(change, 0))
            for m in range(M):
                low = change[m - 1] if m > 0 else 0.0
                high = change[m + 1] if m < M - 1 else 0.0
                near = jnp.where(lane % 2 == 1 - k, low, high)
                total = (X[h + 1, m + 1, row:row + 1] + change[m]) + (near + sums[8 * m:8 * m + 8])
                DY[k, m] = jnp.where(sub == end, total, jnp.where(sub == following, change[m], 0.0)) * f32(SIXTH)
                if ended:
                    DYR[k, m] = jnp.where(sub == end, change[m], 0.0)
        def black(m, tiles):
            value = X[h + 2, m + 1, pl.ds(PAD + 8 * tiles[0], 8 * len(tiles))] + spread(DZ[m], tiles)
            extra = padded(tiles, DY[0, m], DY[1, m])
            if extra is not None:
                value = value + extra
            if m in (0, M - 1):
                value = value + DX[0 if m == 0 else 1, pl.ds(8 * tiles[0], 8 * len(tiles))]
            return value

        def finished(m):
            for tiles in chunks:
                begin, length = 8 * tiles[0], 8 * len(tiles)
                value = black(m, tiles)
                red = X[h + 1, m + 1, pl.ds(PAD + begin, length)] + spread(V[m + 1], tiles)
                extra = padded(tiles, DYR[0, m], DYR[1, m])
                if extra is not None:
                    red = red + extra
                if m in (0, M - 1):
                    red = red + DR[0 if m == 0 else 1, pl.ds(8 + begin, length)]
                obuf[2 * m, pl.ds(begin, length)] = jnp.where(odd_rows[:length], value, red)
                obuf[2 * m + 1, pl.ds(begin, length)] = jnp.where(odd_rows[:length], red, value)

        if ended:
            for m in range(1, M - 1):
                finished(m)
        wait(r, x_faces)
        if r == 0:
            wait(SWEEPS, x_faces)
            for k, plane in enumerate((0, M + 1)):
                half = sxin[k]
                S[0, plane, pl.ds(PAD, N // 2)] = half
                S[0, plane, pl.ds(PAD + N // 2, N // 2)] = pltpu.roll(half, LANES - 1, 1)
        for k, (plane, near) in enumerate(((0, 1), (M + 1, M))):
            for tiles in chunks:
                length = 8 * len(tiles)
                bare = X[h, plane, pl.ds(PAD + 8 * tiles[0], length)] * f32(SIXTH)
                odd = odd_rows[:length]
                DR[k, pl.ds(8 + 8 * tiles[0], length)] = jnp.where(odd, bare, 0.0) if k else jnp.where(odd, 0.0, bare)
            for tiles in chunks:
                begin, length = 8 * tiles[0], 8 * len(tiles)
                here, odd = pl.ds(PAD + begin, length), odd_rows[:length]
                bare = DR[k, pl.ds(8 + begin, length)]
                around = lane_sum(bare) + (DR[k, pl.ds(7 + begin, length)] + DR[k, pl.ds(9 + begin, length)])
                rest = (S[0, plane, here] + X[h, plane, here]) + X[h, near, here]
                rest = rest + jnp.where(outer_rows[:length], wings_of(U[k], tiles), 0.0)
                if tiles[0] == 0:
                    rest = rest + jnp.where(row_of[:length] == 0, X[h, plane, PAD - 1:PAD], 0.0)
                if tiles[-1] == T - 1:
                    rest = rest + jnp.where(row_of[:length] == length - 1, X[h, plane, PAD + N:PAD + N + 1], 0.0)
                red = rest * f32(SIXTH) + around
                red = jnp.where(odd, 0.0, red) if k else jnp.where(odd, red, 0.0)
                DX[k, pl.ds(begin, length)] = (jnp.where(has[k], red, 0.0) + (bare + around)) * f32(SIXTH)
        wait(r, yz_edges)
        small = (M, LANES)
        spot = iota(small, 1) % 4
        ends = (iota(small, 1) == 0) | (iota(small, 1) == LANES - 1)
        low_corner = jnp.where(spot == 1, yzin[r, 0, 0], yzin[r, 0, 1])
        high_corner = jnp.where(spot == 1, yzin[r, 1, 0], yzin[r, 1, 1])
        Y[0] = jnp.where(ends, turn(swapped(low_corner), LANES - 2 - 4 * (T - 1)), 0.0) * f32(1.0 / 18.0)
        Y[1] = jnp.where(ends, turn(swapped(high_corner), LANES - 2), 0.0) * f32(1.0 / 18.0)
        for m in range(M):
            for k, (end, spot) in enumerate(((0, pl.ds(0, 8)), (7, pl.ds(N - 8, 8)))):
                corner = jnp.where(sub == end, Y[k, m:m + 1], 0.0)
                if ended and 0 < m < M - 1:
                    obuf[2 * m, spot] = obuf[2 * m, spot] + jnp.where(odd8, corner, 0.0)
                    obuf[2 * m + 1, spot] = obuf[2 * m + 1, spot] + jnp.where(odd8, 0.0, corner)
                else:
                    DY[k, m] = DY[k, m] + corner

        if not ended:
            for m in (0, M - 1):
                acc = zero8
                for tiles in chunks:
                    value = black(m, tiles)
                    X[h + 2, m + 1, pl.ds(PAD + 8 * tiles[0], 8 * len(tiles))] = value
                    for t in tiles:
                        acc = pack(acc, t, value[8 * (t - tiles[0]):8 * (t - tiles[0]) + 8])
                own[r + 1, m] = acc
            for m in range(1, M - 1):
                for t in (0, T - 1):
                    X[h + 2, m + 1, pl.ds(PAD + 8 * t, 8)] = black(m, [t])
                low = jnp.where(group == 0, turn(DY[0, m], 2), 0.0)
                high = jnp.where(group == T - 1, turn(DY[1, m], 4 * T - 2), 0.0)
                own[r + 1, m] = (PK[m] + DZ[m]) + (low + high)
            finish_pack(r + 1)
            start(r + 1, ordered)
        else:
            finished(0)
            finished(M - 1)

    for r in range(SWEEPS):
        for route in ROUTES:
            guarded(route[0], lambda route=route: remote(r, route).wait_send())
    for route in faces:
        guarded(route[0], lambda route=route: remote(SWEEPS, route).wait_send())


def on_device(field, source):
    L, N, K = field.shape
    M = L // 2
    vmem = lambda *shape: pltpu.VMEM(shape, f32)
    return pl.pallas_call(
        kernel,
        out_shape=jax.ShapeDtypeStruct(field.shape, f32),
        in_specs=[pl.BlockSpec(memory_space=pltpu.HBM)] * 2,
        out_specs=pl.BlockSpec(memory_space=pltpu.VMEM),
        scratch_shapes=[
            vmem(L, N, K), vmem(L, N, K),
            vmem(2, M + 2, N + 2 * PAD, K),
            vmem(HALF + 1, M + 2, N + 2 * PAD, K),
            vmem(SWEEPS, M, 8, K),
            vmem(SWEEPS, 2, M // 2, 8, K),
            vmem(SWEEPS, 2, M // 2, 8, K),
            vmem(SWEEPS, 2, 2, 8, K),
            vmem(SWEEPS, 2, M, K),
            vmem(SWEEPS, 2, 2, M, K),
            vmem(M, 8, K),
            vmem(2, -(-M // 4), 8, K),
            vmem(2, -(-M // 4), 8, K),
            vmem(2, N // 2, K), vmem(2, N // 2, K),
            vmem(M, 8, K),
            vmem(M + 2, 8, K),
            vmem(2, 8, K),
            vmem(2, M, K),
            vmem(M, 8, K),
            vmem(M + 2, 8, K),
            vmem(M, 8, K),
            vmem(M, 8, K),
            vmem(2, M, 8, K),
            vmem(2, M, 8, K),
            vmem(2, N + 16, K),
            vmem(2, N, K),
            pltpu.SemaphoreType.DMA((7,)),
            pltpu.SemaphoreType.DMA((SWEEPS + 1, len(ROUTES))),
            pltpu.SemaphoreType.DMA((SWEEPS + 1, len(ROUTES))),
        ],
        compiler_params=pltpu.CompilerParams(collective_id=0, has_side_effects=True, vmem_limit_bytes=40 << 20),
    )(pltpu.with_memory_space_constraint(field, pltpu.HBM), pltpu.with_memory_space_constraint(source, pltpu.HBM))


def solution(mesh):
    spec = P("gx", "gy", "gz")
    return jax.shard_map(on_device, mesh=mesh, in_specs=(spec, spec), out_specs=spec, check_vma=False)
```
